32 devices in a mesh: front: 8 (over z, y), row: 2 (over core), col: 2 (over x).
Axes of the slice: x: 2, y: 2, z: 4, core: 2. Of those that a mesh axis runs over, the one named last changes fastest.
Arguments:
- bounds: int32 [8], P('front'), may hold values from 3072 to 5120, as said below
- block_map: int32 [8, 40], P('front', 'row'), may hold values from 0 to 383, as said below
- pivot_inverse: bfloat16 [8, 1024, 1024], P('front', 'col', 'row'), may hold values from -0.1875 to 0.1875
- upper_block: bfloat16 [8, 1024, 5120], P('front', 'row', 'col'), may hold values from -0.078125 to 0.078125
- lower_block: bfloat16 [8, 5120, 1024], P('front', 'row', 'col'), may hold values from -0.1875 to 0.1875
- trailing_block: bfloat16 [8, 5120, 5120], P('front', 'row', 'col'), may hold values from -0.078125 to 0.078125
- sketch: bfloat16 [5120, 512], P('col'), may hold values from -6 to 6
- basis: bfloat16 [8, 6144, 512], P('front', 'row'), may hold values from -0.078125 to 0.078125
Outputs:
- coefficients: float32 [8, 512, 512], P('front', None, 'col')
- residual: float32 [8, 6144, 512], P('front', 'row', 'col')
The draws below stay inside these ranges and needn't reach their ends.
Inputs may be any that keep to these rules, and one draw needn't show every extreme that they name: `bounds`: each is a multiple of 128; some front has exactly 5120. `block_map`: entries for blocks at or beyond a front's boundary are ignored. Within one front all entries are distinct. Owner (g, r) holds parent blocks g * 48 + r * 24 to g * 48 + (r + 1) * 24 - 1; an entry held by the device at index r of row names a block of an owner with the same r. Among the 20 entries held by one device, at most 3 name blocks of one owner, and some device has exactly 3 for some owner.
All inputs are finite; a program needn't handle non-finite values.
Results may differ from the reference program's by a relative error of at most 0.0042.
Values may be sent and summed in bfloat16 or wider, within the bound.
No kernel may reach another device: no remote copies, remote signals or barrier semaphores. Data moves between devices by JAX's collectives and lax.ppermute only.
A program may use at most 128 MiB of HBM per device.

```python
import jax
import jax.numpy as jnp
from jax import lax

PIVOT = 1024
BMAX = 5120
BMIN = 3072
BLOCK = 128
SKETCH = 512
RANK = 512
FRONT_DEV = 1
PBLK_DEV = 24
FRONTS = 8
BLK = 40
BLK_DEV = 20
DESTS = 8
CAP = 3
PARENTS = 8
PROWS = 6144


def draw_bounds(key, part):
    block_count = BMAX // BLOCK
    lowest = BMIN // BLOCK
    drawn_blocks = jax.random.randint(jax.random.fold_in(key, 11), (FRONTS,), lowest, block_count + 1)
    widest = jax.random.randint(jax.random.fold_in(key, 12), (), 0, FRONTS)
    chosen = jnp.where(jnp.arange(FRONTS) == widest, block_count, drawn_blocks)
    return (chosen * BLOCK).astype(jnp.int32)


def draw_block_map(key, part):
    order_key = jax.random.fold_in(key, 21)
    row_total = BLK // BLK_DEV
    sender_total = DESTS * row_total

    def shuffle_one(sender_id):
        return jax.random.permutation(jax.random.fold_in(order_key, sender_id), DESTS)
    orders = jax.vmap(shuffle_one)(jnp.arange(sender_total, dtype=jnp.int32)).astype(jnp.int32)
    offsets = jax.random.randint(jax.random.fold_in(key, 22), (FRONTS, DESTS), 0, PBLK_DEV).astype(jnp.int32)
    fronts = jnp.arange(FRONTS, dtype=jnp.int32)[:, None]
    columns = jnp.arange(BLK, dtype=jnp.int32)[None, :]
    row_of = columns // BLK_DEV
    sender = fronts // FRONT_DEV * row_total + row_of
    order_pos = fronts % FRONT_DEV * BLK_DEV + columns % BLK_DEV
    target = orders[sender, order_pos // CAP]
    local_block = (offsets[fronts, target] + order_pos % CAP) % PBLK_DEV
    return (target * (PBLK_DEV * row_total) + row_of * PBLK_DEV + local_block).astype(jnp.int32)


def steps_of(own_key, shape, shards, low, top_value):
    factor_of = 1.0
    for position, shards_of in shards:
        steps = jax.random.uniform(jax.random.fold_in(jax.random.fold_in(own_key, 6), position), (shards_of,), jnp.float32, low / len(shards), top_value / len(shards))
        factor_of = factor_of * jnp.repeat(jnp.exp(steps), shape[position] // shards_of).reshape((-1,) + (1,) * (len(shape) - 1 - position))
    return factor_of


def noise(key, extent, deviation, reach, cuts=(), held_as=jnp.bfloat16):
    entries = deviation * jax.random.normal(key, extent, jnp.float32)
    if cuts:
        entries = entries * steps_of(key, extent, cuts, -0.22, 0.18)
    return jnp.clip(entries, -reach, reach).astype(held_as)


def setup_inputs(seed: int = 0) -> dict:
    streams_of = jax.random.split(jax.random.key(seed), 9)
    return {
        "bounds": draw_bounds(jax.random.fold_in(streams_of[8], 71), 0),
        "block_map": draw_block_map(jax.random.fold_in(streams_of[8], 71), 0),
        "pivot_inverse": noise(streams_of[2], (FRONTS, PIVOT, PIVOT), PIVOT ** -0.5, 0.1875, ((0, 8), (1, 2), (2, 2))),
        "upper_block": noise(streams_of[3], (FRONTS, PIVOT, BMAX), BMAX ** -0.5, 0.078125, ((0, 8), (1, 2), (2, 2))),
        "lower_block": noise(streams_of[4], (FRONTS, BMAX, PIVOT), PIVOT ** -0.5, 0.1875, ((0, 8), (1, 2), (2, 2))),
        "trailing_block": noise(streams_of[5], (FRONTS, BMAX, BMAX), BMAX ** -0.5, 0.078125, ((0, 8), (1, 2), (2, 2))),
        "sketch": noise(streams_of[6], (BMAX, SKETCH), 1.0, 6.0, ((0, 2),)),
        "basis": noise(streams_of[7], (PARENTS, PROWS, RANK), PROWS ** -0.5, 0.078125, ((0, 8), (1, 2))),
    }


def reference(bounds, block_map, pivot_inverse, upper_block, lower_block, trailing_block, sketch, basis):
    positions = jnp.arange(BMAX, dtype=jnp.int32)

    def one_front(pieces):
        boundary, inverse, upper_part, lower_part, trailing = pieces
        masked = sketch * (positions < boundary).astype(jnp.bfloat16)[:, None]
        pivot_rows = jnp.dot(upper_part, masked, preferred_element_type=jnp.float32).astype(jnp.bfloat16)
        solved = jnp.dot(inverse, pivot_rows, preferred_element_type=jnp.float32).astype(jnp.bfloat16)
        return jnp.dot(trailing, masked, preferred_element_type=jnp.float32) - jnp.dot(lower_part, solved, preferred_element_type=jnp.float32)

    sketched = lax.map(one_front, (bounds, pivot_inverse, upper_block, lower_block, trailing_block))
    total_blocks = PARENTS * PROWS // BLOCK
    blocks = sketched.reshape(FRONTS * BLK, BLOCK, SKETCH)
    starts = jnp.arange(BLK, dtype=jnp.int32) * BLOCK
    live_rows = (starts[None, :] < bounds[:, None]).reshape(-1)
    targets = jnp.where(live_rows, block_map.reshape(-1), total_blocks).astype(jnp.int32)
    parent = jnp.zeros((total_blocks, BLOCK, SKETCH), jnp.float32).at[targets].add(blocks, mode="drop")
    parent = parent.reshape(PARENTS, PROWS, SKETCH)
    rounded = lax.optimization_barrier(parent.astype(jnp.bfloat16)).astype(jnp.float32)
    basis_wide = basis.astype(jnp.float32)
    coefficients = jnp.einsum("prq,prk->pqk", basis_wide, rounded, precision=lax.Precision.HIGHEST)
    coeff_rounded = lax.optimization_barrier(coefficients.astype(jnp.bfloat16)).astype(jnp.float32)
    projected = jnp.einsum("prq,pqk->prk", basis_wide, coeff_rounded, precision=lax.Precision.HIGHEST)
    return coefficients, parent - projected
```

```python
import functools

import jax
import jax.numpy as jnp
from jax import lax
from jax.experimental import pallas as pl
from jax.experimental.pallas import tpu as pltpu
from jax.sharding import PartitionSpec as P

BLOCK = 128
TAG_ROWS = 16
F32 = jnp.float32
BF16 = jnp.bfloat16
VMEM = pl.BlockSpec(memory_space=pltpu.VMEM)
SMEM = pl.BlockSpec(memory_space=pltpu.SMEM)
LIMIT = 56 * 1024 * 1024


def cost(flops, nbytes):
    return pl.CostEstimate(flops=int(flops), bytes_accessed=int(nbytes), transcendentals=0)


def params(**kw):
    return pltpu.CompilerParams(vmem_limit_bytes=LIMIT, **kw)


def dot(a, b):
    return jnp.dot(a, b, preferred_element_type=F32)


def mask_halves(bound, col, sketch_ref, out_ref):
    depth, width = sketch_ref.shape
    half = width // 2
    limit = bound - col * depth
    step = 256 if depth % 256 == 0 else depth
    for start in range(0, depth, step):
        rows = pl.ds(start, step)
        at = lax.broadcasted_iota(jnp.int32, (step, half), 0) + start
        for side in range(2):
            pick = col if side == 0 else 1 - col
            value = sketch_ref[rows, pl.ds(pl.multiple_of(pick * half, half), half)]
            value = jnp.where(at < limit, value.astype(F32), 0.0).astype(BF16)
            out_ref[rows, side * half : (side + 1) * half] = value


def plan_kernel(row_count, per_device, cap, fronts, ids_ref, bound_ref, map_ref, pos_ref, tag_ref, count_ref):
    me, row = ids_ref[0], ids_ref[1]
    blocks = map_ref.shape[0]
    slots = fronts * cap
    for i in range(fronts):
        count_ref[i] = 0
    for i in range(slots):
        tag_ref[i] = per_device

    def one(j, carry):
        value = map_ref[j]
        live = (row * blocks + j) * BLOCK < bound_ref[0]
        turn = lax.bitwise_xor(value // (row_count * per_device), me)
        rank = count_ref[turn]
        slot = turn * cap + rank
        pos_ref[j] = jnp.where(live, slot, slots)

        @pl.when(live)
        def _():
            count_ref[turn] = rank + 1
            tag_ref[slot] = value % per_device

        return carry

    lax.fori_loop(0, blocks, one, 0)


def pivot_kernel(ids_ref, bound_ref, upper_ref, sketch_ref, own_ref, other_ref, kept_own_ref, kept_other_ref, masked_ref):
    mask_halves(bound_ref[0], ids_ref[2], sketch_ref, masked_ref)
    half = masked_ref.shape[1] // 2
    own = dot(upper_ref[...], masked_ref[:, :half])
    kept_own_ref[...] = own
    own_ref[...] = own.astype(BF16)
    other = dot(upper_ref[...], masked_ref[:, half:])
    kept_other_ref[...] = other
    other_ref[...] = other.astype(BF16)


def trailing_kernel(ids_ref, bound_ref, trailing_ref, sketch_ref, own_ref, other_ref, masked_ref):
    @pl.when(pl.program_id(0) == 0)
    def _():
        mask_halves(bound_ref[0], ids_ref[2], sketch_ref, masked_ref)

    half = masked_ref.shape[1] // 2
    own_ref[...] = dot(trailing_ref[...], masked_ref[:, :half])
    other_ref[...] = dot(trailing_ref[...], masked_ref[:, half:])


def solve_kernel(inverse_ref, kept_ref, got_ref, out_ref):
    rows = (kept_ref[...] + got_ref[...].astype(F32)).astype(BF16)
    out_ref[...] = dot(inverse_ref[...], rows)


def schur_kernel(groups, cap, pos_ref, part_ref, got_ref, lower_ref, trailing_ref, *rest):
    outs, slots_ref = rest[:-1], rest[-1]
    solved = (part_ref[...] + got_ref[...]).astype(BF16)
    height = lower_ref.shape[0]
    step = 4 * BLOCK if height % (4 * BLOCK) == 0 else BLOCK
    slots_ref[...] = jnp.zeros_like(slots_ref)
    for start in range(0, height, step):
        value = trailing_ref[start : start + step, :] - dot(lower_ref[start : start + step, :], solved)
        for j in range(step // BLOCK):
            at = pos_ref[start // BLOCK + j]
            slots_ref[pl.ds(pl.multiple_of(at * BLOCK, BLOCK), BLOCK), :] = value[j * BLOCK : (j + 1) * BLOCK, :].astype(
                slots_ref.dtype
            )
    size = cap * BLOCK
    for out, turns in zip(outs, groups):
        for i, turn in enumerate(turns):
            out[i * size : (i + 1) * size, :] = slots_ref[turn * size : (turn + 1) * size, :]


def add_kernel(turns, cap, tag_ref, own_ref, got_ref, *outs):
    size = cap * BLOCK
    width = own_ref.shape[1]
    index = lax.broadcasted_iota(jnp.int32, (TAG_ROWS, width), 0)
    for i, (turn, out) in enumerate(zip(turns, outs)):
        rows = slice(i * size, (i + 1) * size)
        out[:size, :] = (own_ref[rows, :] + got_ref[rows, :].astype(F32)).astype(BF16)
        tags = jnp.zeros((TAG_ROWS, width), F32)
        for s in range(cap):
            tags = jnp.where(index == s, tag_ref[turn * cap + s].astype(F32), tags)
        out[size:, :] = tags.astype(BF16)


def gather_kernel(per_device, cap, *refs):
    basis_ref, pieces, (parent_ref, coeff_ref, sum_ref) = refs[0], refs[1:-3], refs[-3:]
    size = cap * BLOCK
    sum_ref[...] = jnp.zeros_like(sum_ref)
    for piece in pieces:
        for s in range(cap):
            tile = piece[size : size + TAG_ROWS, :BLOCK].astype(F32)
            index = lax.broadcasted_iota(jnp.int32, tile.shape, 0)
            tag = jnp.max(jnp.where(index == s, tile, 0.0)).astype(jnp.int32)

            @pl.when(tag < per_device)
            def _():
                at = pl.ds(pl.multiple_of(tag * BLOCK, BLOCK), BLOCK)
                sum_ref[at, :] += piece[s * BLOCK : (s + 1) * BLOCK, :].astype(F32)

    parent_ref[...] = sum_ref[...]
    coeff_ref[...] = lax.dot_general(
        basis_ref[...], sum_ref[...].astype(BF16), (((0,), (0,)), ((), ())), preferred_element_type=F32
    )


def residual_kernel(basis_ref, parent_ref, part_ref, got_ref, coeff_ref, out_ref):
    total = part_ref[...] + got_ref[...]

    @pl.when(pl.program_id(0) == 0)
    def _():
        coeff_ref[...] = total

    out_ref[...] = parent_ref[...] - dot(basis_ref[...], total.astype(BF16))


def swap(x, axis, turn=1):
    n = lax.axis_size(axis)
    return lax.ppermute(x, axis, [(i, i ^ turn) for i in range(n)])


def body(bounds, block_map, pivot_inverse, upper_block, lower_block, trailing_block, sketch, basis):
    fronts, row_count = lax.axis_size("front"), lax.axis_size("row")
    assert fronts & (fronts - 1) == 0
    blocks = block_map.shape[1]
    per_device = basis.shape[1] // BLOCK
    cap = -(-blocks // fronts)
    half = sketch.shape[1] // 2
    depth = sketch.shape[0]
    slots = fronts * cap
    size = cap * BLOCK
    me = lax.axis_index("front")
    ids = jnp.stack([me, lax.axis_index("row"), lax.axis_index("col")]).astype(jnp.int32)
    inverse, upper, lower, trailing, basis = pivot_inverse[0], upper_block[0], lower_block[0], trailing_block[0], basis[0]
    height, pivots = lower.shape

    turns = []
    bit = fronts // 2
    while bit:
        turns += list(range(bit, 2 * bit))
        bit //= 2
    turns.append(0)
    cuts = [0, fronts // 8, fronts // 4, fronts // 2, fronts]
    groups = [turns[a:b] for a, b in zip(cuts, cuts[1:])]

    pos, tags = pl.pallas_call(
        functools.partial(plan_kernel, row_count, per_device, cap, fronts),
        out_shape=(jax.ShapeDtypeStruct((blocks,), jnp.int32), jax.ShapeDtypeStruct((slots,), jnp.int32)),
        in_specs=[SMEM] * 3,
        out_specs=(SMEM, SMEM),
        scratch_shapes=[pltpu.SMEM((fronts,), jnp.int32)],
        cost_estimate=cost(1e6, 1e3),
        name="plan",
    )(ids, bounds, block_map.reshape(-1))

    send_own, send_other, kept_own, kept_other = pl.pallas_call(
        pivot_kernel,
        out_shape=(
            jax.ShapeDtypeStruct((upper.shape[0], half), BF16),
            jax.ShapeDtypeStruct((upper.shape[0], half), BF16),
            jax.ShapeDtypeStruct((upper.shape[0], half), F32),
            jax.ShapeDtypeStruct((upper.shape[0], half), F32),
        ),
        in_specs=[SMEM, SMEM, VMEM, VMEM],
        out_specs=(VMEM,) * 4,
        scratch_shapes=[pltpu.VMEM(sketch.shape, BF16)],
        compiler_params=params(),
        cost_estimate=cost(2 * upper.shape[0] * depth * 2 * half, 2 * upper.size + 2 * sketch.size),
        name="pivot",
    )(ids, bounds, upper, sketch)
    got_other = swap(send_own, "col")
    got_own = swap(send_other, "col")

    tile = 4 * BLOCK if height % (4 * BLOCK) == 0 else BLOCK
    trail_own, trail_other = pl.pallas_call(
        trailing_kernel,
        out_shape=(jax.ShapeDtypeStruct((height, half), F32),) * 2,
        grid=(height // tile,),
        in_specs=[
            SMEM,
            SMEM,
            pl.BlockSpec((tile, depth), lambda i: (i, 0)),
            pl.BlockSpec(sketch.shape, lambda i: (0, 0)),
        ],
        out_specs=(pl.BlockSpec((tile, half), lambda i: (i, 0)),) * 2,
        scratch_shapes=[pltpu.VMEM(sketch.shape, BF16)],
        compiler_params=params(dimension_semantics=("arbitrary",)),
        cost_estimate=cost(2 * height * depth * 2 * half, 2 * trailing.size + 2 * sketch.size + 8 * height * half),
        name="trailing",
    )(ids, bounds, trailing, sketch)

    def solve(kept, got, name):
        return pl.pallas_call(
            solve_kernel,
            out_shape=jax.ShapeDtypeStruct((inverse.shape[0], half), F32),
            in_specs=[VMEM] * 3,
            out_specs=VMEM,
            compiler_params=params(),
            cost_estimate=cost(2 * inverse.size * half, 2 * inverse.size + 6 * kept.size),
            name=name,
        )(inverse, kept, got)

    def schur(part, got, trail, parts, dtype, name):
        return pl.pallas_call(
            functools.partial(schur_kernel, parts, cap),
            out_shape=tuple(jax.ShapeDtypeStruct((len(t) * size, half), dtype) for t in parts),
            in_specs=[SMEM] + [VMEM] * 4,
            out_specs=(VMEM,) * len(parts),
            scratch_shapes=[pltpu.VMEM(((slots + 1) * BLOCK, half), dtype)],
            compiler_params=params(),
            cost_estimate=cost(2 * lower.size * half, 2 * lower.size + 4 * trail.size + 8 * part.size),
            name=name,
        )(pos, part, got, lower, trail)

    part_other = solve(kept_other, got_other, "solve_other")
    sums_other = schur(part_other, swap(part_other, "row"), trail_other, groups, BF16, "schur_other")
    arrived = [swap(x, "col") for x in sums_other]
    part_own = solve(kept_own, got_own, "solve_own")
    sums_own = schur(part_own, swap(part_own, "row"), trail_own, groups, F32, "schur_own")

    pieces = []
    for g, members in enumerate(groups):
        made = pl.pallas_call(
            functools.partial(add_kernel, members, cap),
            out_shape=tuple(jax.ShapeDtypeStruct((size + TAG_ROWS, half), BF16) for _ in members),
            in_specs=[SMEM, VMEM, VMEM],
            out_specs=(VMEM,) * len(members),
            compiler_params=params(),
            cost_estimate=cost(2e9, 8 * len(members) * size * half),
            name=f"add{g}",
        )(tags, sums_own[g], arrived[g])
        for turn, piece in zip(members, made):
            pieces.append(swap(piece, "front", turn) if turn else piece)

    rank = basis.shape[1]
    parent, part = pl.pallas_call(
        functools.partial(gather_kernel, per_device, cap),
        out_shape=(jax.ShapeDtypeStruct((per_device * BLOCK, half), F32), jax.ShapeDtypeStruct((rank, half), F32)),
        in_specs=[VMEM] * (1 + len(pieces)),
        out_specs=(VMEM, VMEM),
        scratch_shapes=[pltpu.VMEM((per_device * BLOCK, half), F32)],
        compiler_params=params(),
        cost_estimate=cost(2 * basis.size * half, 2 * basis.size + 8 * per_device * BLOCK * half),
        name="gather",
    )(basis, *pieces)
    got = swap(part, "row")
    steps = 4 if per_device % 4 == 0 else 1
    tall = per_device * BLOCK // steps
    coefficients, residual = pl.pallas_call(
        residual_kernel,
        out_shape=(jax.ShapeDtypeStruct((rank, half), F32), jax.ShapeDtypeStruct((per_device * BLOCK, half), F32)),
        grid=(steps,),
        in_specs=[
            pl.BlockSpec((tall, rank), lambda i: (i, 0)),
            pl.BlockSpec((tall, half), lambda i: (i, 0)),
            pl.BlockSpec((rank, half), lambda i: (0, 0)),
            pl.BlockSpec((rank, half), lambda i: (0, 0)),
        ],
        out_specs=(pl.BlockSpec((rank, half), lambda i: (0, 0)), pl.BlockSpec((tall, half), lambda i: (i, 0))),
        compiler_params=params(dimension_semantics=("arbitrary",)),
        cost_estimate=cost(2 * basis.size * half, 2 * basis.size + 8 * per_device * BLOCK * half),
        name="residual",
    )(basis, parent, part, got)
    return coefficients[None], residual[None]


def solution(mesh):
    placed = (
        P("front"),
        P("front", "row"),
        P("front", "col", "row"),
        P("front", "row", "col"),
        P("front", "row", "col"),
        P("front", "row", "col"),
        P("col", None),
        P("front", "row", None),
    )
    return jax.shard_map(
        body,
        mesh=mesh,
        in_specs=placed,
        out_specs=(P("front", None, "col"), P("front", "row", "col")),
        check_vma=False,
    )
```

```python
import functools

import jax
import jax.numpy as jnp
from jax import lax
from jax.experimental import pallas as pl
from jax.experimental.pallas import tpu as pltpu
from jax.sharding import PartitionSpec as P


BLOCK = 128
TAG_ROWS = 16
F32 = jnp.float32
BF16 = jnp.bfloat16
VMEM = pl.BlockSpec(memory_space=pltpu.VMEM)
SMEM = pl.BlockSpec(memory_space=pltpu.SMEM)
MIB = 1024 * 1024
PIVOT_LIMIT = 16 * MIB
TRAILING_LIMIT = 46 * MIB


def dot(a, b):
    return jnp.dot(a, b, preferred_element_type=F32)


def mask_halves(bound, first, col, sketch_ref, out_ref):
    depth, width = sketch_ref.shape
    half = width // 2
    limit = bound - first * depth
    at = lax.broadcasted_iota(jnp.int32, (depth, half), 0)
    for side in range(2):
        pick = col if side == 0 else 1 - col
        value = sketch_ref[:, pl.ds(pl.multiple_of(pick * half, half), half)]
        out_ref[:, side * half : (side + 1) * half] = jnp.where(at < limit, value.astype(F32), 0.0).astype(BF16)


def plan_kernel(row_count, per_device, cap, fronts, ids_ref, bound_ref, map_ref, source_ref, tag_ref, count_ref):
    me, row = ids_ref[0], ids_ref[1]
    blocks = map_ref.shape[0]
    slots = fronts * cap
    for i in range(fronts):
        count_ref[i] = 0
    for i in range(slots):
        source_ref[i] = 0
        tag_ref[i] = per_device

    def one(j, carry):
        value = map_ref[j]

        @pl.when((row * blocks + j) * BLOCK < bound_ref[0])
        def _():
            turn = lax.bitwise_xor(value // (row_count * per_device), me)
            rank = count_ref[turn]
            count_ref[turn] = rank + 1
            source_ref[turn * cap + rank] = j
            tag_ref[turn * cap + rank] = value % per_device

        return carry

    lax.fori_loop(0, blocks, one, 0)


def pivot_kernel(ids_ref, bound_ref, upper_ref, sketch_ref, own_ref, other_ref, kept_own_ref, kept_other_ref, masked_ref, sum_ref):
    step, steps = pl.program_id(0), pl.num_programs(0)
    half = sketch_ref.shape[1] // 2
    mask_halves(bound_ref[0], ids_ref[2] * steps + step, ids_ref[2], sketch_ref, masked_ref)
    value = dot(upper_ref[...], masked_ref[...])

    @pl.when(step == 0)
    def _():
        sum_ref[...] = value

    @pl.when(step > 0)
    def _():
        sum_ref[...] += value

    @pl.when(step == steps - 1)
    def _():
        kept_own_ref[...] = sum_ref[:, :half]
        own_ref[...] = sum_ref[:, :half].astype(BF16)
        kept_other_ref[...] = sum_ref[:, half:]
        other_ref[...] = sum_ref[:, half:].astype(BF16)


def trailing_kernel(trailing_ref, masked_ref, own_ref, other_ref):
    value = dot(trailing_ref[...], masked_ref[...])
    half = masked_ref.shape[1] // 2
    own_ref[...] = value[:, :half]
    other_ref[...] = value[:, half:]


def solve_kernel(inverse_ref, kept_ref, got_ref, out_ref):
    rows = (kept_ref[...] + got_ref[...].astype(F32)).astype(BF16)
    out_ref[...] = dot(inverse_ref[...], rows)


def schur_kernel(part_ref, got_ref, lower_ref, trailing_ref, out_ref):
    solved = (part_ref[...] + got_ref[...]).astype(BF16)
    height = lower_ref.shape[0]
    step = 4 * BLOCK if height % (4 * BLOCK) == 0 else BLOCK
    for start in range(0, height, step):
        rows = slice(start, start + step)
        out_ref[rows, :] = (trailing_ref[rows, :] - dot(lower_ref[rows, :], solved)).astype(out_ref.dtype)


def packed_schur_kernel(groups, cap, source_ref, part_ref, got_ref, lower_ref, trailing_ref, *rest):
    outs, sum_ref = rest[:-1], rest[-1]
    schur_kernel(part_ref, got_ref, lower_ref, trailing_ref, sum_ref)
    for out, turns in zip(outs, groups):
        for i, turn in enumerate(turns):
            for s in range(cap):
                at = pl.multiple_of(source_ref[turn * cap + s] * BLOCK, BLOCK)
                start = (i * cap + s) * BLOCK
                out[start : start + BLOCK, :] = sum_ref[pl.ds(at, BLOCK), :]


def add_kernel(turns, cap, source_ref, tag_ref, own_ref, got_ref, *outs):
    size = cap * BLOCK
    width = own_ref.shape[1]
    index = lax.broadcasted_iota(jnp.int32, (TAG_ROWS, width), 0)
    for i, (turn, out) in enumerate(zip(turns, outs)):
        tags = jnp.zeros((TAG_ROWS, width), F32)
        for s in range(cap):
            at = pl.multiple_of(source_ref[turn * cap + s] * BLOCK, BLOCK)
            start = i * size + s * BLOCK
            value = own_ref[pl.ds(at, BLOCK), :] + got_ref[start : start + BLOCK, :].astype(F32)
            out[s * BLOCK : (s + 1) * BLOCK, :] = value.astype(BF16)
            tags = jnp.where(index == s, tag_ref[turn * cap + s].astype(F32), tags)
        out[size:, :] = tags.astype(BF16)


def add_pieces(per_device, cap, pieces, parent_ref):
    size = cap * BLOCK
    for piece in pieces:
        tile = piece[size : size + TAG_ROWS, :BLOCK].astype(F32)
        index = lax.broadcasted_iota(jnp.int32, tile.shape, 0)
        for s in range(cap):
            tag = jnp.max(jnp.where(index == s, tile, 0.0)).astype(jnp.int32)

            @pl.when(tag < per_device)
            def _():
                at = pl.ds(pl.multiple_of(tag * BLOCK, BLOCK), BLOCK)
                parent_ref[at, :] += piece[s * BLOCK : (s + 1) * BLOCK, :].astype(F32)


def early_kernel(per_device, cap, *refs):
    pieces, parent_ref = refs[:-1], refs[-1]
    parent_ref[...] = jnp.zeros_like(parent_ref)
    add_pieces(per_device, cap, pieces, parent_ref)


def late_kernel(per_device, cap, *refs):
    flipped_ref, pieces, (parent_ref, coeff_ref) = refs[0], refs[2:-2], refs[-2:]
    add_pieces(per_device, cap, pieces, parent_ref)
    coeff_ref[...] = dot(flipped_ref[...], parent_ref[...].astype(BF16))


def flip_kernel(basis_ref, out_ref):
    out_ref[...] = basis_ref[...].T


def residual_kernel(basis_ref, parent_ref, part_ref, got_ref, coeff_ref, out_ref):
    total = part_ref[...] + got_ref[...]

    @pl.when(pl.program_id(0) == 0)
    def _():
        coeff_ref[...] = total

    out_ref[...] = parent_ref[...] - dot(basis_ref[...], total.astype(BF16))


def swap(x, axis, turn=1):
    n = lax.axis_size(axis)
    return lax.ppermute(x, axis, [(i, i ^ turn) for i in range(n)])


def order_of(fronts):
    turns = []
    bit = fronts // 2
    while bit:
        turns += list(range(bit, 2 * bit))
        bit //= 2
    turns.append(0)
    cuts = [0, fronts // 8, fronts // 4, fronts // 2, fronts]
    return turns, [turns[a:b] for a, b in zip(cuts, cuts[1:])]


def call(kernel, operands, specs, outs, out_specs, flops, scratch=(), limit=None, **kw):
    space = 0
    for x in (*operands, *outs, *scratch):
        space += x.size * x.dtype.itemsize if hasattr(x, "size") else 0
    moved = sum(x.size * x.dtype.itemsize for x in (*operands, *outs))
    semantics = {"dimension_semantics": ("arbitrary",)} if "grid" in kw else {}
    return pl.pallas_call(
        kernel,
        out_shape=tuple(outs),
        in_specs=specs,
        out_specs=tuple(out_specs),
        scratch_shapes=[pltpu.VMEM(x.shape, x.dtype) if isinstance(x, jax.ShapeDtypeStruct) else x for x in scratch],
        compiler_params=pltpu.CompilerParams(vmem_limit_bytes=int(limit or space + 3 * MIB), **semantics),
        cost_estimate=pl.CostEstimate(flops=int(flops), bytes_accessed=int(moved), transcendentals=0),
        **kw,
    )(*operands)


def shape(rows, columns, dtype):
    return jax.ShapeDtypeStruct((rows, columns), dtype)


def program(bounds, block_map, pivot_inverse, upper_block, lower_block, trailing_block, sketch, basis):
    fronts, row_count = lax.axis_size("front"), lax.axis_size("row")
    assert fronts & (fronts - 1) == 0
    blocks = block_map.shape[1]
    per_device = basis.shape[1] // BLOCK
    cap = -(-blocks // fronts)
    depth, width = sketch.shape
    half = width // 2
    slots = fronts * cap
    size = cap * BLOCK
    ids = jnp.stack([lax.axis_index("front"), lax.axis_index("row"), lax.axis_index("col")]).astype(jnp.int32)
    inverse, upper, lower, trailing, basis = pivot_inverse[0], upper_block[0], lower_block[0], trailing_block[0], basis[0]
    height, _ = lower.shape
    tall = upper.shape[0]
    turns, groups = order_of(fronts)

    steps = 5 if depth % (5 * BLOCK) == 0 else 1
    part = depth // steps
    send_own, send_other, kept_own, kept_other, masked = call(
        pivot_kernel,
        (ids, bounds, upper, sketch),
        [
            SMEM,
            SMEM,
            pl.BlockSpec((tall, part), lambda k: (0, k)),
            pl.BlockSpec((part, width), lambda k: (k, 0)),
        ],
        (shape(tall, half, BF16),) * 2 + (shape(tall, half, F32),) * 2 + (shape(depth, width, BF16),),
        [pl.BlockSpec((tall, half), lambda k: (0, 0))] * 4 + [pl.BlockSpec((part, width), lambda k: (k, 0))],
        2 * upper.size * width,
        scratch=(shape(tall, width, F32),),
        limit=PIVOT_LIMIT,
        grid=(steps,),
    )
    got_other = swap(send_own, "col")
    got_own = swap(send_other, "col")

    source, tags = call(
        functools.partial(plan_kernel, row_count, per_device, cap, fronts),
        (ids, bounds, block_map.reshape(-1)),
        [SMEM] * 3,
        (jax.ShapeDtypeStruct((slots,), jnp.int32),) * 2,
        [SMEM] * 2,
        1e6,
        scratch=(pltpu.SMEM((fronts,), jnp.int32),),
    )

    tile = 4 * BLOCK if height % (4 * BLOCK) == 0 else BLOCK
    trail_own, trail_other = call(
        trailing_kernel,
        (trailing, masked),
        [pl.BlockSpec((tile, depth), lambda i: (i, 0)), pl.BlockSpec((depth, width), lambda i: (0, 0))],
        (shape(height, half, F32),) * 2,
        [pl.BlockSpec((tile, half), lambda i: (i, 0))] * 2,
        2 * trailing.size * width,
        limit=TRAILING_LIMIT,
        grid=(height // tile,),
    )

    def solve(kept, got):
        return call(solve_kernel, (inverse, kept, got), [VMEM] * 3, (shape(inverse.shape[0], half, F32),), [VMEM], 2 * inverse.size * half)[0]

    part_other = solve(kept_other, got_other)
    row_other = swap(part_other, "row")
    part_own = solve(kept_own, got_own)
    row_own = swap(part_own, "row")
    sums = call(
        functools.partial(packed_schur_kernel, groups, cap),
        (source, part_other, row_other, lower, trail_other),
        [SMEM] + [VMEM] * 4,
        tuple(shape(len(t) * size, half, BF16) for t in groups),
        [VMEM] * len(groups),
        2 * lower.size * half,
        scratch=(shape(height, half, BF16),),
    )
    arrived = [swap(x, "col") for x in sums]
    own = call(
        schur_kernel,
        (part_own, row_own, lower, trail_own),
        [VMEM] * 4,
        (shape(height, half, F32),),
        [VMEM],
        2 * lower.size * half,
    )[0]

    pieces = {}
    for g, members in enumerate(groups):
        made = call(
            functools.partial(add_kernel, members, cap),
            (source, tags, own, arrived[g]),
            [SMEM, SMEM, VMEM, VMEM],
            (shape(size + TAG_ROWS, half, BF16),) * len(members),
            [VMEM] * len(members),
            1e9,
        )
        for turn, piece in zip(members, made):
            pieces[turn] = swap(piece, "front", turn) if turn else piece

    rank = basis.shape[1]
    rows = per_device * BLOCK
    flipped = call(flip_kernel, (basis,), [VMEM], (shape(rank, rows, BF16),), [VMEM], 1e9)[0]
    late = groups[2]
    early = [t for t in turns if t not in late]
    parent = call(
        functools.partial(early_kernel, per_device, cap),
        [pieces[t] for t in early],
        [VMEM] * len(early),
        (shape(rows, half, F32),),
        [VMEM],
        1e9,
    )[0]
    parent, coeff = call(
        functools.partial(late_kernel, per_device, cap),
        [flipped, parent] + [pieces[t] for t in late],
        [VMEM] * (2 + len(late)),
        (shape(rows, half, F32), shape(rank, half, F32)),
        [VMEM] * 2,
        2 * basis.size * half,
        input_output_aliases={1: 0},
    )
    got = swap(coeff, "row")
    steps = 4 if per_device % 4 == 0 else 1
    tall = rows // steps
    coefficients, residual = call(
        residual_kernel,
        (basis, parent, coeff, got),
        [
            pl.BlockSpec((tall, rank), lambda i: (i, 0)),
            pl.BlockSpec((tall, half), lambda i: (i, 0)),
            pl.BlockSpec((rank, half), lambda i: (0, 0)),
            pl.BlockSpec((rank, half), lambda i: (0, 0)),
        ],
        (shape(rank, half, F32), shape(rows, half, F32)),
        [pl.BlockSpec((rank, half), lambda i: (0, 0)), pl.BlockSpec((tall, half), lambda i: (i, 0))],
        2 * basis.size * half,
        grid=(steps,),
        limit=20 * MIB,
    )
    return coefficients[None], residual[None]


def solution(mesh):
    placed = (
        P("front"),
        P("front", "row"),
        P("front", "col", "row"),
        P("front", "row", "col"),
        P("front", "row", "col"),
        P("front", "row", "col"),
        P("col", None),
        P("front", "row", None),
    )
    return jax.shard_map(
        program,
        mesh=mesh,
        in_specs=placed,
        out_specs=(P("front", None, "col"), P("front", "row", "col")),
        check_vma=False,
    )
```

```python
import functools

import jax
import jax.numpy as jnp
from jax import lax
from jax.experimental import pallas as pl
from jax.experimental.pallas import tpu as pltpu
from jax.sharding import PartitionSpec as P


BLOCK = 128
TAG_ROWS = 8
F32 = jnp.float32
BF16 = jnp.bfloat16
VMEM = pl.BlockSpec(memory_space=pltpu.VMEM)
SMEM = pl.BlockSpec(memory_space=pltpu.SMEM)
MIB = 1024 * 1024
TRAILING_LIMIT = 22 * MIB
ANY = pl.BlockSpec(memory_space=pl.ANY)


def dot(a, b):
    return jnp.dot(a, b, preferred_element_type=F32)


def pivot_kernel(
    sizes, ids_ref, bound_ref, map_ref, upper_hbm, sketch_hbm,
    own_ref, other_ref, kept_own_ref, kept_other_ref, masked_ref, order_ref, offset_ref, tag_ref,
    upper_ref, sketch_ref, sum_ref, upper_sem, sketch_sem, count_ref, rank_ref,
):
    depth, width = sketch_ref.shape
    half = width // 2
    parts = upper_sem.shape[0]
    part = depth // parts
    copies = []
    for k in range(parts):
        at = pl.ds(k * part, part)
        copies.append(
            (
                pltpu.make_async_copy(upper_hbm.at[:, at], upper_ref.at[:, at], upper_sem.at[k]),
                pltpu.make_async_copy(sketch_hbm.at[at, :], sketch_ref.at[at, :], sketch_sem.at[k]),
            )
        )
        for copy in copies[-1]:
            copy.start()
    plan(*sizes, ids_ref, bound_ref, map_ref, order_ref, offset_ref, tag_ref, count_ref, rank_ref)
    col = ids_ref[2]
    for k in range(parts):
        for copy in copies[k]:
            copy.wait()
        for start in range(k * part, (k + 1) * part, BLOCK):
            rows = slice(start, start + BLOCK)
            keep = jnp.where(col * depth + start < bound_ref[0], 1.0, 0.0).astype(F32)
            keep = jnp.full((BLOCK, half), keep, F32).astype(BF16)
            for side in range(2):
                pick = col if side == 0 else 1 - col
                value = sketch_ref[rows, pl.ds(pl.multiple_of(pick * half, half), half)]
                masked_ref[rows, side * half : (side + 1) * half] = value * keep
        first = (parts + 1) // 2
        if k == first - 1:
            at = slice(0, first * part)
            sum_ref[...] = dot(upper_ref[:, at], masked_ref[at, :])
        if k == parts - 1 and parts > 1:
            at = slice(first * part, depth)
            sum_ref[...] += dot(upper_ref[:, at], masked_ref[at, :])
    kept_own_ref[...] = sum_ref[:, :half]
    own_ref[...] = sum_ref[:, :half].astype(BF16)
    kept_other_ref[...] = sum_ref[:, half:]
    other_ref[...] = sum_ref[:, half:].astype(BF16)


def trailing_kernel(trailing_ref, masked_ref, own_ref, other_ref):
    value = dot(trailing_ref[...], masked_ref[...])
    half = masked_ref.shape[1] // 2
    own_ref[...] = value[:, :half]
    other_ref[...] = value[:, half:]


def solve_kernel(inverse_ref, kept_ref, got_ref, out_ref):
    rows = (kept_ref[...] + got_ref[...].astype(F32)).astype(BF16)
    out_ref[...] = dot(inverse_ref[...], rows)


def schur_kernel(part_ref, got_ref, lower_ref, trailing_ref, out_ref):
    solved = (part_ref[...] + got_ref[...]).astype(BF16)
    height = lower_ref.shape[0]
    step = 4 * BLOCK if height % (4 * BLOCK) == 0 else BLOCK
    for start in range(0, height, step):
        rows = slice(start, start + step)
        out_ref[rows, :] = (trailing_ref[rows, :] - dot(lower_ref[rows, :], solved)).astype(out_ref.dtype)


def packed_schur_kernel(cuts, order_ref, part_ref, got_ref, lower_ref, trailing_ref, *rest):
    outs, sum_ref = rest[:-1], rest[-1]
    schur_kernel(part_ref, got_ref, lower_ref, trailing_ref, sum_ref)
    for out, first in zip(outs, cuts):
        for p in range(out.shape[0] // BLOCK):
            at = pl.multiple_of(order_ref[first + p] * BLOCK, BLOCK)
            out[p * BLOCK : (p + 1) * BLOCK, :] = sum_ref[pl.ds(at, BLOCK), :]


def add_kernel(keys, cap, first, count, fresh, order_ref, offset_ref, tag_ref, own_ref, *refs):
    refs = list(refs)
    got_ref = refs.pop(0) if count else None
    if not fresh:
        refs.pop(0)
    sum_ref, outs = refs[0], refs[1:]
    for p in range(count):
        at = pl.multiple_of(order_ref[first + p] * BLOCK, BLOCK)
        value = own_ref[pl.ds(at, BLOCK), :] + got_ref[p * BLOCK : (p + 1) * BLOCK, :].astype(F32)
        sum_ref[(first + p) * BLOCK : (first + p + 1) * BLOCK, :] = value.astype(BF16)
    size = cap * BLOCK
    last = sum_ref.shape[0] // BLOCK - 1
    index = lax.broadcasted_iota(jnp.int32, (TAG_ROWS, sum_ref.shape[1]), 0)
    for key, out in zip(keys, outs):
        tags = jnp.zeros(index.shape, F32)
        for s in range(cap):
            at = pl.multiple_of(jnp.minimum(offset_ref[key] + s, last) * BLOCK, BLOCK)
            out[s * BLOCK : (s + 1) * BLOCK, :] = sum_ref[pl.ds(at, BLOCK), :]
            tags = jnp.where(index == s, tag_ref[key * cap + s].astype(F32), tags)
        out[size:, :] = tags.astype(BF16)


def add_pieces(per_device, cap, pieces, parent_ref):
    size = cap * BLOCK
    for piece in pieces:
        tile = piece[size : size + TAG_ROWS, :BLOCK].astype(F32)
        index = lax.broadcasted_iota(jnp.int32, tile.shape, 0)
        for s in range(cap):
            tag = jnp.max(jnp.where(index == s, tile, 0.0)).astype(jnp.int32)

            @pl.when(tag < per_device)
            def _():
                at = pl.ds(pl.multiple_of(tag * BLOCK, BLOCK), BLOCK)
                parent_ref[at, :] += piece[s * BLOCK : (s + 1) * BLOCK, :].astype(F32)


def early_kernel(per_device, cap, fresh, *refs):
    pieces, parent_ref = refs[: -1 if fresh else -2], refs[-1]
    if fresh:
        parent_ref[...] = jnp.zeros_like(parent_ref)
    add_pieces(per_device, cap, pieces, parent_ref)


def late_kernel(per_device, cap, *refs):
    flipped_ref, pieces, (parent_ref, coeff_ref) = refs[0], refs[2:-2], refs[-2:]
    add_pieces(per_device, cap, pieces, parent_ref)
    coeff_ref[...] = dot(flipped_ref[...], parent_ref[...].astype(BF16))


def flip_kernel(basis_ref, out_ref):
    out_ref[...] = basis_ref[...].T


def residual_kernel(basis_ref, parent_ref, part_ref, got_ref, coeff_hbm, out_hbm, coeff_ref, out_ref, coeff_sem, out_sem):
    total = part_ref[...] + got_ref[...]
    coeff_ref[...] = total
    copies = [pltpu.make_async_copy(coeff_ref, coeff_hbm, coeff_sem)]
    copies[0].start()
    total = total.astype(BF16)
    parts = out_sem.shape[0]
    part = out_ref.shape[0] // parts
    for k in range(parts):
        rows = slice(k * part, (k + 1) * part)
        out_ref[rows, :] = parent_ref[rows, :] - dot(basis_ref[rows, :], total)
        at = pl.ds(k * part, part)
        copies.append(pltpu.make_async_copy(out_ref.at[at, :], out_hbm.at[at, :], out_sem.at[k]))
        copies[-1].start()
    for copy in copies:
        copy.wait()


def swap(x, axis, turn=1):
    n = lax.axis_size(axis)
    return lax.ppermute(x, axis, [(i, i ^ turn) for i in range(n)])


def order_of(fronts):
    cuts = [0, fronts // 8, fronts // 4, fronts // 2, 3 * fronts // 4, fronts]
    return [list(range(a, b)) for a, b in zip(cuts, cuts[1:])]


def plan(row_count, per_device, cap, fronts, ids_ref, bound_ref, map_ref, order_ref, offset_ref, tag_ref, count_ref, rank_ref):
    me, row = ids_ref[0], ids_ref[1]
    blocks = map_ref.shape[0]
    for i in range(fronts):
        count_ref[i] = 0
    for i in range(fronts * cap):
        tag_ref[i] = per_device
    for i in range(blocks):
        order_ref[i] = 0

    def each_live(one):
        def step(j, carry):
            @pl.when((row * blocks + j) * BLOCK < bound_ref[0])
            def _():
                value = map_ref[j]
                one(j, value, fronts - 1 - lax.bitwise_xor(lax.div(value, row_count * per_device), me))

            return carry

        lax.fori_loop(0, blocks, step, 0)

    def count(j, value, key):
        rank = count_ref[key]
        count_ref[key] = rank + 1
        rank_ref[j] = rank
        tag_ref[key * cap + rank] = lax.rem(value, per_device)

    def place(j, value, key):
        order_ref[offset_ref[key] + rank_ref[j]] = j

    each_live(count)
    start = jnp.int32(0)
    for i in range(fronts):
        offset_ref[i] = start
        start = start + count_ref[i]
    each_live(place)


def call(kernel, operands, specs, outs, out_specs, flops, scratch=(), limit=None, **kw):
    space = 0
    for x in (*operands, *outs, *scratch):
        space += x.size * x.dtype.itemsize if hasattr(x, "size") else 0
    moved = sum(x.size * x.dtype.itemsize for x in (*operands, *outs))
    semantics = {"dimension_semantics": ("arbitrary",)} if "grid" in kw else {}
    return pl.pallas_call(
        kernel,
        out_shape=tuple(outs),
        in_specs=specs,
        out_specs=tuple(out_specs),
        scratch_shapes=[pltpu.VMEM(x.shape, x.dtype) if isinstance(x, jax.ShapeDtypeStruct) else x for x in scratch],
        compiler_params=pltpu.CompilerParams(vmem_limit_bytes=int(limit or space + 3 * MIB), **semantics),
        cost_estimate=pl.CostEstimate(flops=int(flops), bytes_accessed=int(moved), transcendentals=0),
        **kw,
    )(*operands)


def in_hbm(x):
    return pltpu.with_memory_space_constraint(x, pltpu.HBM)


def shape(rows, columns, dtype):
    return jax.ShapeDtypeStruct((rows, columns), dtype)


def program(bounds, block_map, pivot_inverse, upper_block, lower_block, trailing_block, sketch, basis):
    fronts, row_count = lax.axis_size("front"), lax.axis_size("row")
    assert fronts & (fronts - 1) == 0
    blocks = block_map.shape[1]
    per_device = basis.shape[1] // BLOCK
    cap = -(-blocks // fronts)
    depth, width = sketch.shape
    half = width // 2
    size = cap * BLOCK
    ids = jnp.stack([lax.axis_index("front"), lax.axis_index("row"), lax.axis_index("col")]).astype(jnp.int32)
    inverse, upper, lower, trailing, basis = pivot_inverse[0], upper_block[0], lower_block[0], trailing_block[0], basis[0]
    height, _ = lower.shape
    tall = upper.shape[0]
    groups = order_of(fronts)

    steps = 5 if depth % (5 * BLOCK) == 0 else 1
    send_own, send_other, kept_own, kept_other, masked, order, offset, tags = call(
        functools.partial(pivot_kernel, (row_count, per_device, cap, fronts)),
        (ids, bounds, block_map.reshape(-1), in_hbm(upper), in_hbm(sketch)),
        [SMEM, SMEM, SMEM, ANY, ANY],
        (shape(tall, half, BF16),) * 2
        + (shape(tall, half, F32),) * 2
        + (shape(depth, width, BF16),)
        + tuple(jax.ShapeDtypeStruct((n,), jnp.int32) for n in (blocks, fronts, fronts * cap)),
        [VMEM] * 5 + [SMEM] * 3,
        2 * upper.size * width,
        scratch=(
            shape(tall, depth, BF16),
            shape(depth, width, BF16),
            shape(tall, width, F32),
            pltpu.SemaphoreType.DMA((steps,)),
            pltpu.SemaphoreType.DMA((steps,)),
            pltpu.SMEM((fronts,), jnp.int32),
            pltpu.SMEM((blocks,), jnp.int32),
        ),
    )
    got_other = swap(send_own, "col")
    got_own = swap(send_other, "col")

    tile = 4 * BLOCK if height % (4 * BLOCK) == 0 else BLOCK
    trail_own, trail_other = call(
        trailing_kernel,
        (in_hbm(trailing), masked),
        [pl.BlockSpec((tile, depth), lambda i: (i, 0)), pl.BlockSpec((depth, width), lambda i: (0, 0))],
        (shape(height, half, F32),) * 2,
        [pl.BlockSpec((tile, half), lambda i: (i, 0))] * 2,
        2 * trailing.size * width,
        limit=TRAILING_LIMIT,
        grid=(height // tile,),
    )

    def solve(kept, got):
        return call(solve_kernel, (inverse, kept, got), [VMEM] * 3, (shape(inverse.shape[0], half, F32),), [VMEM], 2 * inverse.size * half)[0]

    part_other = solve(kept_other, got_other)
    row_other = swap(part_other, "row")
    part_own = solve(kept_own, got_own)
    row_own = swap(part_own, "row")
    cuts = [0] + [min(cap * (g[-1] + 1), blocks) for g in groups]
    counts = [b - a for a, b in zip(cuts, cuts[1:])]
    sums = call(
        functools.partial(packed_schur_kernel, [a for a, n in zip(cuts, counts) if n]),
        (order, part_other, row_other, lower, trail_other),
        [SMEM] + [VMEM] * 4,
        tuple(shape(n * BLOCK, half, BF16) for n in counts if n),
        [VMEM] * sum(n > 0 for n in counts),
        2 * lower.size * half,
        scratch=(shape(height, half, BF16),),
    )
    arrived = [swap(x, "col") for x in sums]
    own = call(
        schur_kernel,
        (part_own, row_own, lower, trail_own),
        [VMEM] * 4,
        (shape(height, half, F32),),
        [VMEM],
        2 * lower.size * half,
    )[0]

    pieces = {}
    total = None
    for g, keys in enumerate(groups):
        operands = [order, offset, tags, own]
        if counts[g]:
            operands.append(arrived[g])
        if g:
            operands.append(total)
        total, *made = call(
            functools.partial(add_kernel, keys, cap, cuts[g], counts[g], g == 0),
            operands,
            [SMEM] * 3 + [VMEM] * (len(operands) - 3),
            (shape(blocks * BLOCK, half, BF16),) + (shape(size + TAG_ROWS, half, BF16),) * len(keys),
            [VMEM] * (1 + len(keys)),
            1e9,
            **({"input_output_aliases": {len(operands) - 1: 0}} if g else {}),
        )
        for key, piece in zip(keys, made):
            turn = fronts - 1 - key
            pieces[key] = swap(piece, "front", turn) if turn else piece

    rank = basis.shape[1]
    rows = per_device * BLOCK
    flipped = call(flip_kernel, (basis,), [VMEM], (shape(rank, rows, BF16),), [VMEM], 1e9)[0]
    waves = [[fronts - 1] + groups[0] + groups[1], groups[2], [k for g in groups[3:] for k in g if k < fronts - 1]]
    parent = call(
        functools.partial(early_kernel, per_device, cap, True),
        [pieces[k] for k in waves[0]],
        [VMEM] * len(waves[0]),
        (shape(rows, half, F32),),
        [VMEM],
        1e9,
    )[0]
    parent = call(
        functools.partial(early_kernel, per_device, cap, False),
        [pieces[k] for k in waves[1]] + [parent],
        [VMEM] * (1 + len(waves[1])),
        (shape(rows, half, F32),),
        [VMEM],
        1e9,
        input_output_aliases={len(waves[1]): 0},
    )[0]
    parent, coeff = call(
        functools.partial(late_kernel, per_device, cap),
        [flipped, parent] + [pieces[k] for k in waves[2]],
        [VMEM] * (2 + len(waves[2])),
        (shape(rows, half, F32), shape(rank, half, F32)),
        [VMEM] * 2,
        2 * basis.size * half,
        input_output_aliases={1: 0},
    )
    got = swap(coeff, "row")
    steps = 6 if per_device % 6 == 0 else 1
    coefficients, residual = call(
        residual_kernel,
        (basis, parent, coeff, got),
        [VMEM] * 4,
        (shape(rank, half, F32), shape(rows, half, F32)),
        [ANY] * 2,
        2 * basis.size * half,
        scratch=(
            shape(rank, half, F32),
            shape(rows, half, F32),
            pltpu.SemaphoreType.DMA,
            pltpu.SemaphoreType.DMA((steps,)),
        ),
    )
    return coefficients[None], residual[None]


def solution(mesh):
    placed = (
        P("front"),
        P("front", "row"),
        P("front", "col", "row"),
        P("front", "row", "col"),
        P("front", "row", "col"),
        P("front", "row", "col"),
        P("col", None),
        P("front", "row", None),
    )

    def step(*args):
        sharded = jax.shard_map(
            program,
            mesh=mesh,
            in_specs=placed,
            out_specs=(P("front", None, "col"), P("front", "row", "col")),
            check_vma=False,
        )
        return sharded(*args)

    return step
```

```python
import functools

import jax
import jax.numpy as jnp
from jax import lax
from jax.experimental import pallas as pl
from jax.experimental.pallas import tpu as pltpu
from jax.sharding import PartitionSpec as P


BLOCK = 128
TAG_ROWS = 8
F32 = jnp.float32
BF16 = jnp.bfloat16
VMEM = pl.BlockSpec(memory_space=pltpu.VMEM)
SMEM = pl.BlockSpec(memory_space=pltpu.SMEM)
MIB = 1024 * 1024
ANY = pl.BlockSpec(memory_space=pl.ANY)


def dot(a, b):
    return jnp.dot(a, b, preferred_element_type=F32)


def pivot_kernel(
    sizes, ids_ref, bound_ref, map_hbm, upper_hbm, sketch_hbm, trailing_hbm,
    own_ref, other_ref, kept_own_ref, kept_other_ref, masked_ref, head_ref, order_ref, offset_ref, tag_ref,
    upper_ref, sketch_ref, sum_ref, upper_sem, sketch_sem, head_sem, map_sem, map_ref, count_ref, rank_ref, key_ref,
):
    map_copy = pltpu.make_async_copy(map_hbm, map_ref, map_sem)
    map_copy.start()
    depth, width = sketch_ref.shape
    half = width // 2
    parts = upper_sem.shape[0]
    part = depth // parts
    copies = []
    for k in range(parts):
        at = pl.ds(k * part, part)
        copies.append(
            (
                pltpu.make_async_copy(upper_hbm.at[:, at], upper_ref.at[:, at], upper_sem.at[k]),
                pltpu.make_async_copy(sketch_hbm.at[at, :], sketch_ref.at[at, :], sketch_sem.at[k]),
            )
        )
        for copy in copies[-1]:
            copy.start()
    head_copy = pltpu.make_async_copy(trailing_hbm.at[pl.ds(0, head_ref.shape[0]), :], head_ref, head_sem)
    head_copy.start()
    map_copy.wait()
    plan(*sizes, ids_ref, bound_ref, map_ref, order_ref, offset_ref, tag_ref, count_ref, rank_ref, key_ref)
    col = ids_ref[2]
    for k in range(parts):
        for copy in copies[k]:
            copy.wait()
        for start in range(k * part, (k + 1) * part, BLOCK):
            rows = slice(start, start + BLOCK)
            keep = jnp.where(col * depth + start < bound_ref[0], 1.0, 0.0).astype(F32)
            keep = jnp.full((BLOCK, half), keep, F32).astype(BF16)
            for side in range(2):
                pick = col if side == 0 else 1 - col
                value = sketch_ref[rows, pl.ds(pl.multiple_of(pick * half, half), half)]
                masked_ref[rows, side * half : (side + 1) * half] = value * keep
        first = (parts + 1) // 2
        if k == first - 1:
            at = slice(0, first * part)
            sum_ref[...] = dot(upper_ref[:, at], masked_ref[at, :])
        if k == parts - 1 and parts > 1:
            at = slice(first * part, depth)
            sum_ref[...] += dot(upper_ref[:, at], masked_ref[at, :])
    kept_own_ref[...] = sum_ref[:, :half]
    own_ref[...] = sum_ref[:, :half].astype(BF16)
    kept_other_ref[...] = sum_ref[:, half:]
    other_ref[...] = sum_ref[:, half:].astype(BF16)
    head_copy.wait()


def trailing_kernel(tile, trailing_hbm, head_ref, masked_ref, own_ref, other_ref, rest_ref, rest_sem):
    height, half = own_ref.shape
    head = head_ref.shape[0]
    copies = []
    for i, start in enumerate(range(head, height, tile)):
        copies.append(
            pltpu.make_async_copy(
                trailing_hbm.at[pl.ds(start, tile), :], rest_ref.at[pl.ds(start - head, tile), :], rest_sem.at[i]
            )
        )
        copies[-1].start()
    for start in range(0, height, tile):
        rows = slice(start, start + tile)
        if start < head:
            value = dot(head_ref[rows, :], masked_ref[...])
        else:
            copies[(start - head) // tile].wait()
            value = dot(rest_ref[start - head : start - head + tile, :], masked_ref[...])
        own_ref[rows, :] = value[:, :half]
        other_ref[rows, :] = value[:, half:]


def solve_kernel(inverse_ref, kept_ref, got_ref, out_ref):
    rows = (kept_ref[...] + got_ref[...].astype(F32)).astype(BF16)
    out_ref[...] = dot(inverse_ref[...], rows)


def schur_kernel(part_ref, got_ref, lower_ref, trailing_ref, out_ref):
    solved = (part_ref[...] + got_ref[...]).astype(BF16)
    height = lower_ref.shape[0]
    step = 4 * BLOCK if height % (4 * BLOCK) == 0 else BLOCK
    for start in range(0, height, step):
        rows = slice(start, start + step)
        out_ref[rows, :] = (trailing_ref[rows, :] - dot(lower_ref[rows, :], solved)).astype(out_ref.dtype)


def first_schur_kernel(order_ref, part_ref, got_ref, lower_ref, trailing_ref, out_ref):
    solved = (part_ref[...] + got_ref[...]).astype(BF16)
    for p in range(out_ref.shape[0] // BLOCK):
        at = pl.ds(pl.multiple_of(order_ref[p] * BLOCK, BLOCK), BLOCK)
        value = trailing_ref[at, :] - dot(lower_ref[at, :], solved)
        out_ref[p * BLOCK : (p + 1) * BLOCK, :] = value.astype(BF16)


def packed_schur_kernel(cuts, order_ref, part_ref, got_ref, lower_ref, trailing_ref, *rest):
    outs, sum_ref = rest[:-1], rest[-1]
    schur_kernel(part_ref, got_ref, lower_ref, trailing_ref, sum_ref)
    for out, first in zip(outs, cuts):
        for p in range(out.shape[0] // BLOCK):
            at = pl.multiple_of(order_ref[first + p] * BLOCK, BLOCK)
            out[p * BLOCK : (p + 1) * BLOCK, :] = sum_ref[pl.ds(at, BLOCK), :]


def add_kernel(
    parts, cap, first, count, fresh, order_ref, offset_ref, tag_ref, part_ref, row_ref, lower_ref, trailing_ref, *refs
):
    refs = list(refs)
    got_ref = refs.pop(0) if count else None
    if not fresh:
        refs.pop(0)
    sum_ref, outs = refs[0], refs[1:]
    solved = (part_ref[...] + row_ref[...]).astype(BF16)
    for p in range(count):
        at = pl.ds(pl.multiple_of(order_ref[first + p] * BLOCK, BLOCK), BLOCK)
        value = trailing_ref[at, :] - dot(lower_ref[at, :], solved) + got_ref[p * BLOCK : (p + 1) * BLOCK, :].astype(F32)
        sum_ref[(first + p) * BLOCK : (first + p + 1) * BLOCK, :] = value.astype(BF16)
    last = sum_ref.shape[0] // BLOCK - 1
    index = lax.broadcasted_iota(jnp.int32, (TAG_ROWS, sum_ref.shape[1]), 0)
    for (key, low, high), out in zip(parts, outs):
        tags = jnp.zeros(index.shape, F32)
        for s in range(low, high):
            at = pl.multiple_of(jnp.minimum(offset_ref[key] + s, last) * BLOCK, BLOCK)
            out[(s - low) * BLOCK : (s - low + 1) * BLOCK, :] = sum_ref[pl.ds(at, BLOCK), :]
            tags = jnp.where(index == s - low, tag_ref[key * cap + s].astype(F32), tags)
        out[(high - low) * BLOCK :, :] = tags.astype(BF16)


def add_pieces(per_device, pieces, parent_ref):
    for piece in pieces:
        count = piece.shape[0] // BLOCK
        tile = piece[count * BLOCK : count * BLOCK + TAG_ROWS, :BLOCK].astype(F32)
        index = lax.broadcasted_iota(jnp.int32, tile.shape, 0)
        for s in range(count):
            tag = jnp.max(jnp.where(index == s, tile, 0.0)).astype(jnp.int32)

            @pl.when(tag < per_device)
            def _():
                at = pl.ds(pl.multiple_of(tag * BLOCK, BLOCK), BLOCK)
                parent_ref[at, :] += piece[s * BLOCK : (s + 1) * BLOCK, :].astype(F32)


def early_kernel(per_device, fresh, *refs):
    pieces, parent_ref = refs[: -1 if fresh else -2], refs[-1]
    if fresh:
        parent_ref[...] = jnp.zeros_like(parent_ref)
    add_pieces(per_device, pieces, parent_ref)


def late_kernel(per_device, *refs):
    flipped_ref, pieces, (parent_ref, coeff_ref) = refs[0], refs[2:-2], refs[-2:]
    add_pieces(per_device, pieces, parent_ref)
    coeff_ref[...] = dot(flipped_ref[...], parent_ref[...].astype(BF16))


def flip_kernel(basis_ref, out_ref):
    out_ref[...] = basis_ref[...].T


def residual_kernel(basis_ref, parent_ref, part_ref, got_ref, coeff_hbm, out_hbm, coeff_ref, out_ref, coeff_sem, out_sem):
    total = part_ref[...] + got_ref[...]
    coeff_ref[...] = total
    copies = [pltpu.make_async_copy(coeff_ref, coeff_hbm, coeff_sem)]
    copies[0].start()
    total = total.astype(BF16)
    parts = out_sem.shape[0]
    part = out_ref.shape[0] // parts
    for k in range(parts):
        rows = slice(k * part, (k + 1) * part)
        out_ref[rows, :] = parent_ref[rows, :] - dot(basis_ref[rows, :], total)
        at = pl.ds(k * part, part)
        copies.append(pltpu.make_async_copy(out_ref.at[at, :], out_hbm.at[at, :], out_sem.at[k]))
        copies[-1].start()
    for copy in copies:
        copy.wait()


def swap(x, axis):
    return lax.ppermute(x, axis, [(i, i ^ 1) for i in range(lax.axis_size(axis))])


def away(x, key, fronts):
    return lax.ppermute(
        x, "front", [(i, j) for i in range(fronts) for j in range(fronts) if key_of(j, i, fronts) == key]
    )


def groups_of(fronts, cap):
    total = fronts * cap
    cuts = [0, 1, total // 8, total // 4, 3 * total // 8, total // 2, 3 * total // 4, total]
    groups = []
    for a, b in zip(cuts, cuts[1:]):
        keys = range(a // cap, -(-b // cap))
        groups.append([(k, max(a - k * cap, 0), min(b - k * cap, cap)) for k in keys if b > a])
    return groups, cuts


LEGS = (2, 1, 3, 0)


def gray(x):
    return x ^ (x >> 1)


def key_of(owner, me, fronts):
    inner = fronts // 4
    leg = (gray(owner // inner) - gray(me // inner)) & 3 if isinstance(owner, int) else lax.bitwise_and(
        gray_of(lax.div(owner, inner)) - gray_of(lax.div(me, inner)) + 4, 3
    )
    rest = inner - 1 - ((owner ^ me) & (inner - 1))
    if isinstance(owner, int):
        return LEGS.index(leg) * inner + rest
    turn = jnp.where(leg == LEGS[0], 0, jnp.where(leg == LEGS[1], 1, jnp.where(leg == LEGS[2], 2, 3)))
    return turn * inner + rest


def gray_of(x):
    return lax.bitwise_xor(x, lax.shift_right_logical(x, jnp.int32(1)))


def divider(by, top):
    for shift in range(8, 31):
        factor = -(-(1 << shift) // by)
        if all(n * factor >> shift == n // by for n in range(top + 1)):
            assert top * factor < 1 << 31
            return factor, shift
    raise ValueError(by)


def plan(row_count, per_device, cap, fronts, ids_ref, bound_ref, map_ref, order_ref, offset_ref, tag_ref, count_ref, rank_ref, key_ref):
    me, row = ids_ref[0], ids_ref[1]
    blocks = map_ref.shape[0]
    factor, shift = divider(per_device, fronts * row_count * per_device)
    assert row_count & (row_count - 1) == 0
    inner = fronts // 4

    def zero(i, carry):
        count_ref[i] = 0
        return carry

    def no_tag(i, carry):
        tag_ref[i] = per_device
        return carry

    def rank_one(j, carry):
        value = map_ref[j]
        holder = lax.shift_right_logical(value * factor, jnp.int32(shift))
        owner = lax.shift_right_logical(holder, jnp.int32(row_count.bit_length() - 1))
        there, here = (lax.shift_right_logical(x, jnp.int32(inner.bit_length() - 1)) for x in (owner, me))
        there, here = (lax.bitwise_xor(x, lax.shift_right_logical(x, jnp.int32(1))) for x in (there, here))
        leg = lax.bitwise_and(there - here, jnp.int32(3))
        turn = jnp.where(leg == LEGS[0], 0, jnp.where(leg == LEGS[1], 1, jnp.where(leg == LEGS[2], 2, 3)))
        key = turn * inner + (inner - 1) - lax.bitwise_and(lax.bitwise_xor(owner, me), jnp.int32(inner - 1))
        key = jnp.where((row * blocks + j) * BLOCK < bound_ref[0], key, fronts)
        rank = count_ref[key]
        count_ref[key] = rank + 1
        rank_ref[j] = rank
        key_ref[j] = key
        tag_ref[key * cap + rank] = value - holder * per_device
        return carry

    def start(i, total):
        offset_ref[i] = total
        return total + count_ref[i]

    def place(j, carry):
        order_ref[offset_ref[key_ref[j]] + rank_ref[j]] = j
        return carry

    lax.fori_loop(0, fronts + 1, zero, 0)
    lax.fori_loop(0, fronts * cap, no_tag, 0)
    lax.fori_loop(0, blocks, rank_one, 0)
    lax.fori_loop(0, fronts + 1, start, jnp.int32(0))
    lax.fori_loop(0, blocks, place, 0)


def call(kernel, operands, specs, outs, out_specs, flops, scratch=(), limit=None, **kw):
    space = 0
    for x in (*operands, *outs, *scratch):
        space += x.size * x.dtype.itemsize if hasattr(x, "size") else 0
    moved = sum(x.size * x.dtype.itemsize for x in (*operands, *outs))
    semantics = {"dimension_semantics": ("arbitrary",)} if "grid" in kw else {}
    return pl.pallas_call(
        kernel,
        out_shape=tuple(outs),
        in_specs=specs,
        out_specs=tuple(out_specs),
        scratch_shapes=[pltpu.VMEM(x.shape, x.dtype) if isinstance(x, jax.ShapeDtypeStruct) else x for x in scratch],
        compiler_params=pltpu.CompilerParams(vmem_limit_bytes=int(limit or space + 3 * MIB), **semantics),
        cost_estimate=pl.CostEstimate(flops=int(flops), bytes_accessed=int(moved), transcendentals=0),
        **kw,
    )(*operands)


def in_hbm(x):
    return pltpu.with_memory_space_constraint(x, pltpu.HBM)


def shape(rows, columns, dtype):
    return jax.ShapeDtypeStruct((rows, columns), dtype)


def program(bounds, block_map, pivot_inverse, upper_block, lower_block, trailing_block, sketch, basis):
    fronts, row_count = lax.axis_size("front"), lax.axis_size("row")
    assert fronts % 4 == 0 and fronts & (fronts - 1) == 0
    blocks = block_map.shape[1]
    per_device = basis.shape[1] // BLOCK
    cap = -(-blocks // fronts)
    depth, width = sketch.shape
    half = width // 2
    ids = jnp.stack([lax.axis_index("front"), lax.axis_index("row"), lax.axis_index("col")]).astype(jnp.int32)
    inverse, upper, lower, trailing, basis = pivot_inverse[0], upper_block[0], lower_block[0], trailing_block[0], basis[0]
    height, _ = lower.shape
    tall = upper.shape[0]
    groups, cuts = groups_of(fronts, cap)

    steps = 5 if depth % (5 * BLOCK) == 0 else 1
    tile = 4 * BLOCK if height % (4 * BLOCK) == 0 else BLOCK
    head = max(height // tile * 2 // 5, 1) * tile
    send_own, send_other, kept_own, kept_other, masked, top, order, offset, tags = call(
        functools.partial(pivot_kernel, (row_count, per_device, cap, fronts)),
        (ids, bounds, in_hbm(block_map.reshape(-1)), in_hbm(upper), in_hbm(sketch), in_hbm(trailing)),
        [SMEM, SMEM, ANY, ANY, ANY, ANY],
        (shape(tall, half, BF16),) * 2
        + (shape(tall, half, F32),) * 2
        + (shape(depth, width, BF16), shape(head, depth, BF16))
        + tuple(jax.ShapeDtypeStruct((n,), jnp.int32) for n in (blocks, fronts + 1, fronts * cap + blocks)),
        [VMEM] * 6 + [SMEM] * 3,
        2 * upper.size * width,
        scratch=(
            shape(tall, depth, BF16),
            shape(depth, width, BF16),
            shape(tall, width, F32),
            pltpu.SemaphoreType.DMA((steps,)),
            pltpu.SemaphoreType.DMA((steps,)),
            pltpu.SemaphoreType.DMA,
            pltpu.SemaphoreType.DMA,
            pltpu.SMEM((blocks,), jnp.int32),
            pltpu.SMEM((fronts + 1,), jnp.int32),
            pltpu.SMEM((blocks,), jnp.int32),
            pltpu.SMEM((blocks,), jnp.int32),
        ),
    )
    got_other = swap(send_own, "col")
    got_own = swap(send_other, "col")

    trail_own, trail_other = call(
        functools.partial(trailing_kernel, tile),
        (in_hbm(trailing), top, masked),
        [ANY, VMEM, VMEM],
        (shape(height, half, F32),) * 2,
        [VMEM] * 2,
        2 * trailing.size * width,
        scratch=(shape(height - head, depth, BF16), pltpu.SemaphoreType.DMA(((height - head) // tile,))),
    )

    def solve(kept, got):
        return call(solve_kernel, (inverse, kept, got), [VMEM] * 3, (shape(inverse.shape[0], half, F32),), [VMEM], 2 * inverse.size * half)[0]

    part_other = solve(kept_other, got_other)
    row_other = swap(part_other, "row")
    cuts = [min(c, blocks) for c in cuts]
    counts = [b - a for a, b in zip(cuts, cuts[1:])]
    sums = call(
        first_schur_kernel,
        (order, part_other, row_other, lower, trail_other),
        [SMEM] + [VMEM] * 4,
        (shape(counts[0] * BLOCK, half, BF16),),
        [VMEM],
        2 * lower.size * half,
    )
    sums += call(
        functools.partial(packed_schur_kernel, [a for a, n in zip(cuts[1:], counts[1:]) if n]),
        (order, part_other, row_other, lower, trail_other),
        [SMEM] + [VMEM] * 4,
        tuple(shape(n * BLOCK, half, BF16) for n in counts[1:] if n),
        [VMEM] * sum(n > 0 for n in counts[1:]),
        2 * lower.size * half,
        scratch=(shape(height, half, BF16),),
    )
    arrived = [swap(x, "col") for x in sums]
    part_own = solve(kept_own, got_own)
    row_own = swap(part_own, "row")

    pieces = []
    total = None
    for g, parts in enumerate(groups):
        if not parts:
            continue
        operands = [order, offset, tags, part_own, row_own, lower, trail_own]
        if counts[g]:
            operands.append(arrived[g])
        if g:
            operands.append(total)
        total, *made = call(
            functools.partial(add_kernel, parts, cap, cuts[g], counts[g], g == 0),
            operands,
            [SMEM] * 3 + [VMEM] * (len(operands) - 3),
            (shape(blocks * BLOCK, half, BF16),)
            + tuple(shape((high - low) * BLOCK + TAG_ROWS, half, BF16) for _, low, high in parts),
            [VMEM] * (1 + len(parts)),
            1e9,
            **({"input_output_aliases": {len(operands) - 1: 0}} if g else {}),
        )
        for (key, _, _), piece in zip(parts, made):
            pieces.append(away(piece, key, fronts) if key < fronts - 1 else piece)

    rank = basis.shape[1]
    rows = per_device * BLOCK
    flipped = call(flip_kernel, (basis,), [VMEM], (shape(rank, rows, BF16),), [VMEM], 1e9)[0]
    counted = [len(g) for g in groups]
    far = sum(counted[:3])
    near = far + sum(counted[3:5])
    end = near + counted[5]
    late = [near - 1, end - 1]
    waves = [[len(pieces) - 1] + list(range(far))]
    waves += [[i for i in range(far, len(pieces) - 1) if i not in late], late]
    parent = None
    for w, keys in enumerate(waves[:-1]):
        parent = call(
            functools.partial(early_kernel, per_device, w == 0),
            [pieces[k] for k in keys] + ([parent] if w else []),
            [VMEM] * (len(keys) + (w > 0)),
            (shape(rows, half, F32),),
            [VMEM],
            1e9,
            **({"input_output_aliases": {len(keys): 0}} if w else {}),
        )[0]
    parent, coeff = call(
        functools.partial(late_kernel, per_device),
        [flipped, parent] + [pieces[k] for k in waves[-1]],
        [VMEM] * (2 + len(waves[-1])),
        (shape(rows, half, F32), shape(rank, half, F32)),
        [VMEM] * 2,
        2 * basis.size * half,
        input_output_aliases={1: 0},
    )
    got = swap(coeff, "row")
    steps = 6 if per_device % 6 == 0 else 1
    coefficients, residual = call(
        residual_kernel,
        (basis, parent, coeff, got),
        [VMEM] * 4,
        (shape(rank, half, F32), shape(rows, half, F32)),
        [ANY] * 2,
        2 * basis.size * half,
        scratch=(
            shape(rank, half, F32),
            shape(rows, half, F32),
            pltpu.SemaphoreType.DMA,
            pltpu.SemaphoreType.DMA((steps,)),
        ),
    )
    return coefficients[None], residual[None]


def solution(mesh):
    placed = (
        P("front"),
        P("front", "row"),
        P("front", "col", "row"),
        P("front", "row", "col"),
        P("front", "row", "col"),
        P("front", "row", "col"),
        P("col", None),
        P("front", "row", None),
    )

    def step(*args):
        sharded = jax.shard_map(
            program,
            mesh=mesh,
            in_specs=placed,
            out_specs=(P("front", None, "col"), P("front", "row", "col")),
            check_vma=False,
        )
        return sharded(*args)

    return step
```

```python
import functools

import jax
import jax.numpy as jnp
from jax import lax
from jax.experimental import pallas as pl
from jax.experimental.pallas import tpu as pltpu
from jax.sharding import PartitionSpec as P


BLOCK = 128
TAG_ROWS = 8
F32 = jnp.float32
BF16 = jnp.bfloat16
VMEM = pl.BlockSpec(memory_space=pltpu.VMEM)
SMEM = pl.BlockSpec(memory_space=pltpu.SMEM)
MIB = 1024 * 1024
ANY = pl.BlockSpec(memory_space=pl.ANY)


def dot(a, b):
    return jnp.dot(a, b, preferred_element_type=F32)


def pivot_kernel(
    sizes, ids_ref, bound_ref, map_hbm, upper_hbm, sketch_hbm, trailing_hbm,
    own_ref, other_ref, kept_own_ref, kept_other_ref, masked_ref, head_ref, order_ref, offset_ref, tag_ref,
    upper_ref, sketch_ref, sum_ref, upper_sem, sketch_sem, head_sem, map_sem, map_ref, count_ref, rank_ref, key_ref,
):
    map_copy = pltpu.make_async_copy(map_hbm, map_ref, map_sem)
    map_copy.start()
    depth, width = sketch_ref.shape
    half = width // 2
    parts = upper_sem.shape[0]
    part = depth // parts
    copies = []
    for k in range(parts):
        at = pl.ds(k * part, part)
        copies.append(
            (
                pltpu.make_async_copy(upper_hbm.at[:, at], upper_ref.at[:, at], upper_sem.at[k]),
                pltpu.make_async_copy(sketch_hbm.at[at, :], sketch_ref.at[at, :], sketch_sem.at[k]),
            )
        )
        for copy in copies[-1]:
            copy.start()
    head_copy = pltpu.make_async_copy(trailing_hbm.at[pl.ds(0, head_ref.shape[0]), :], head_ref, head_sem)
    head_copy.start()
    map_copy.wait()
    plan(*sizes, ids_ref, bound_ref, map_ref, order_ref, offset_ref, tag_ref, count_ref, rank_ref, key_ref)
    col = ids_ref[2]
    for k in range(parts):
        for copy in copies[k]:
            copy.wait()
        for start in range(k * part, (k + 1) * part, BLOCK):
            rows = slice(start, start + BLOCK)
            keep = jnp.where(col * depth + start < bound_ref[0], 1.0, 0.0).astype(F32)
            keep = jnp.full((BLOCK, half), keep, F32).astype(BF16)
            for side in range(2):
                pick = col if side == 0 else 1 - col
                value = sketch_ref[rows, pl.ds(pl.multiple_of(pick * half, half), half)]
                masked_ref[rows, side * half : (side + 1) * half] = value * keep
        first = (parts + 1) // 2
        if k == first - 1:
            at = slice(0, first * part)
            sum_ref[...] = dot(upper_ref[:, at], masked_ref[at, :])
        if k == parts - 1 and parts > 1:
            at = slice(first * part, depth)
            sum_ref[...] += dot(upper_ref[:, at], masked_ref[at, :])
    kept_own_ref[...] = sum_ref[:, :half]
    own_ref[...] = sum_ref[:, :half].astype(BF16)
    kept_other_ref[...] = sum_ref[:, half:]
    other_ref[...] = sum_ref[:, half:].astype(BF16)
    head_copy.wait()


def trailing_kernel(tile, trailing_hbm, head_ref, masked_ref, own_ref, other_ref, rest_ref, rest_sem):
    height, half = own_ref.shape
    head = head_ref.shape[0]
    copies = []
    for i, start in enumerate(range(head, height, tile)):
        copies.append(
            pltpu.make_async_copy(
                trailing_hbm.at[pl.ds(start, tile), :], rest_ref.at[pl.ds(start - head, tile), :], rest_sem.at[i]
            )
        )
        copies[-1].start()
    for start in range(0, height, tile):
        rows = slice(start, start + tile)
        if start < head:
            value = dot(head_ref[rows, :], masked_ref[...])
        else:
            copies[(start - head) // tile].wait()
            value = dot(rest_ref[start - head : start - head + tile, :], masked_ref[...])
        own_ref[rows, :] = value[:, :half]
        other_ref[rows, :] = value[:, half:]


def solve_kernel(inverse_ref, kept_ref, got_ref, out_ref):
    rows = (kept_ref[...] + got_ref[...].astype(F32)).astype(BF16)
    out_ref[...] = dot(inverse_ref[...], rows)


def schur_kernel(part_ref, got_ref, lower_ref, trailing_ref, out_ref):
    solved = (part_ref[...] + got_ref[...]).astype(BF16)
    height = lower_ref.shape[0]
    step = 4 * BLOCK if height % (4 * BLOCK) == 0 else BLOCK
    for start in range(0, height, step):
        rows = slice(start, start + step)
        out_ref[rows, :] = (trailing_ref[rows, :] - dot(lower_ref[rows, :], solved)).astype(out_ref.dtype)


def first_schur_kernel(order_ref, part_ref, got_ref, lower_ref, trailing_ref, out_ref):
    solved = (part_ref[...] + got_ref[...]).astype(BF16)
    for p in range(out_ref.shape[0] // BLOCK):
        at = pl.ds(pl.multiple_of(order_ref[p] * BLOCK, BLOCK), BLOCK)
        value = trailing_ref[at, :] - dot(lower_ref[at, :], solved)
        out_ref[p * BLOCK : (p + 1) * BLOCK, :] = value.astype(BF16)


def packed_schur_kernel(cuts, order_ref, part_ref, got_ref, lower_ref, trailing_ref, *rest):
    outs, sum_ref = rest[:-1], rest[-1]
    schur_kernel(part_ref, got_ref, lower_ref, trailing_ref, sum_ref)
    for out, first in zip(outs, cuts):
        for p in range(out.shape[0] // BLOCK):
            at = pl.multiple_of(order_ref[first + p] * BLOCK, BLOCK)
            out[p * BLOCK : (p + 1) * BLOCK, :] = sum_ref[pl.ds(at, BLOCK), :]


def add_kernel(
    parts, cap, first, count, fresh, order_ref, offset_ref, tag_ref, part_ref, row_ref, lower_ref, trailing_ref, *refs
):
    refs = list(refs)
    got_ref = refs.pop(0) if count else None
    if not fresh:
        refs.pop(0)
    sum_ref, outs = refs[0], refs[1:]
    solved = (part_ref[...] + row_ref[...]).astype(BF16)
    for p in range(count):
        at = pl.ds(pl.multiple_of(order_ref[first + p] * BLOCK, BLOCK), BLOCK)
        value = trailing_ref[at, :] - dot(lower_ref[at, :], solved) + got_ref[p * BLOCK : (p + 1) * BLOCK, :].astype(F32)
        sum_ref[(first + p) * BLOCK : (first + p + 1) * BLOCK, :] = value.astype(BF16)
    last = sum_ref.shape[0] // BLOCK - 1
    index = lax.broadcasted_iota(jnp.int32, (TAG_ROWS, sum_ref.shape[1]), 0)
    for (key, low, high), out in zip(parts, outs):
        tags = jnp.zeros(index.shape, F32)
        for s in range(low, high):
            at = pl.multiple_of(jnp.minimum(offset_ref[key] + s, last) * BLOCK, BLOCK)
            out[(s - low) * BLOCK : (s - low + 1) * BLOCK, :] = sum_ref[pl.ds(at, BLOCK), :]
            tags = jnp.where(index == s - low, tag_ref[key * cap + s].astype(F32), tags)
        out[(high - low) * BLOCK :, :] = tags.astype(BF16)


def add_pieces(per_device, pieces, parent_ref):
    for piece in pieces:
        count = piece.shape[0] // BLOCK
        tile = piece[count * BLOCK : count * BLOCK + TAG_ROWS, :BLOCK].astype(F32)
        index = lax.broadcasted_iota(jnp.int32, tile.shape, 0)
        for s in range(count):
            tag = jnp.max(jnp.where(index == s, tile, 0.0)).astype(jnp.int32)

            @pl.when(tag < per_device)
            def _():
                at = pl.ds(pl.multiple_of(tag * BLOCK, BLOCK), BLOCK)
                parent_ref[at, :] += piece[s * BLOCK : (s + 1) * BLOCK, :].astype(F32)


def early_kernel(per_device, fresh, *refs):
    pieces, parent_ref = refs[: -1 if fresh else -2], refs[-1]
    if fresh:
        parent_ref[...] = jnp.zeros_like(parent_ref)
    add_pieces(per_device, pieces, parent_ref)


def late_kernel(per_device, *refs):
    flipped_ref, pieces, (parent_ref, coeff_ref) = refs[0], refs[2:-2], refs[-2:]
    add_pieces(per_device, pieces, parent_ref)
    coeff_ref[...] = dot(flipped_ref[...], parent_ref[...].astype(BF16))


def flip_kernel(basis_ref, out_ref):
    out_ref[...] = basis_ref[...].T


def residual_kernel(basis_ref, parent_ref, part_ref, got_ref, coeff_hbm, out_hbm, coeff_ref, out_ref, coeff_sem, out_sem):
    total = part_ref[...] + got_ref[...]
    coeff_ref[...] = total
    copies = [pltpu.make_async_copy(coeff_ref, coeff_hbm, coeff_sem)]
    copies[0].start()
    total = total.astype(BF16)
    parts = out_sem.shape[0]
    part = out_ref.shape[0] // parts
    for k in range(parts):
        rows = slice(k * part, (k + 1) * part)
        out_ref[rows, :] = parent_ref[rows, :] - dot(basis_ref[rows, :], total)
        at = pl.ds(k * part, part)
        copies.append(pltpu.make_async_copy(out_ref.at[at, :], out_hbm.at[at, :], out_sem.at[k]))
        copies[-1].start()
    for copy in copies:
        copy.wait()


def swap(x, axis):
    return lax.ppermute(x, axis, [(i, i ^ 1) for i in range(lax.axis_size(axis))])


def away(x, key, fronts):
    return lax.ppermute(
        x, "front", [(i, j) for i in range(fronts) for j in range(fronts) if key_of(j, i, fronts) == key]
    )


def groups_of(fronts, cap):
    total = fronts * cap
    cuts = [0, 2, total // 8, total // 4, 3 * total // 8, total // 2, 3 * total // 4, total]
    groups = []
    for a, b in zip(cuts, cuts[1:]):
        keys = range(a // cap, -(-b // cap))
        groups.append([(k, max(a - k * cap, 0), min(b - k * cap, cap)) for k in keys if b > a])
    return groups, cuts


LEGS = (2, 1, 3, 0)


def gray(x):
    return x ^ (x >> 1)


def key_of(owner, me, fronts):
    inner = fronts // 4
    leg = (gray(owner // inner) - gray(me // inner)) & 3 if isinstance(owner, int) else lax.bitwise_and(
        gray_of(lax.div(owner, inner)) - gray_of(lax.div(me, inner)) + 4, 3
    )
    rest = inner - 1 - ((owner ^ me) & (inner - 1))
    if isinstance(owner, int):
        return LEGS.index(leg) * inner + rest
    turn = jnp.where(leg == LEGS[0], 0, jnp.where(leg == LEGS[1], 1, jnp.where(leg == LEGS[2], 2, 3)))
    return turn * inner + rest


def gray_of(x):
    return lax.bitwise_xor(x, lax.shift_right_logical(x, jnp.int32(1)))


def divider(by, top):
    for shift in range(8, 31):
        factor = -(-(1 << shift) // by)
        if all(n * factor >> shift == n // by for n in range(top + 1)):
            assert top * factor < 1 << 31
            return factor, shift
    raise ValueError(by)


def plan(row_count, per_device, cap, fronts, ids_ref, bound_ref, map_ref, order_ref, offset_ref, tag_ref, count_ref, rank_ref, key_ref):
    me, row = ids_ref[0], ids_ref[1]
    blocks = map_ref.shape[0]
    factor, shift = divider(per_device, fronts * row_count * per_device)
    assert row_count & (row_count - 1) == 0
    inner = fronts // 4

    def zero(i, carry):
        count_ref[i] = 0
        return carry

    def no_tag(i, carry):
        tag_ref[i] = per_device
        return carry

    def rank_one(j, carry):
        value = map_ref[j]
        holder = lax.shift_right_logical(value * factor, jnp.int32(shift))
        owner = lax.shift_right_logical(holder, jnp.int32(row_count.bit_length() - 1))
        there, here = (lax.shift_right_logical(x, jnp.int32(inner.bit_length() - 1)) for x in (owner, me))
        there, here = (lax.bitwise_xor(x, lax.shift_right_logical(x, jnp.int32(1))) for x in (there, here))
        leg = lax.bitwise_and(there - here, jnp.int32(3))
        turn = jnp.where(leg == LEGS[0], 0, jnp.where(leg == LEGS[1], 1, jnp.where(leg == LEGS[2], 2, 3)))
        key = turn * inner + (inner - 1) - lax.bitwise_and(lax.bitwise_xor(owner, me), jnp.int32(inner - 1))
        key = jnp.where((row * blocks + j) * BLOCK < bound_ref[0], key, fronts)
        rank = count_ref[key]
        count_ref[key] = rank + 1
        rank_ref[j] = rank
        key_ref[j] = key
        tag_ref[key * cap + rank] = value - holder * per_device
        return carry

    def start(i, total):
        offset_ref[i] = total
        return total + count_ref[i]

    def place(j, carry):
        order_ref[offset_ref[key_ref[j]] + rank_ref[j]] = j
        return carry

    lax.fori_loop(0, fronts + 1, zero, 0)
    lax.fori_loop(0, fronts * cap, no_tag, 0)
    lax.fori_loop(0, blocks, rank_one, 0)
    lax.fori_loop(0, fronts + 1, start, jnp.int32(0))
    lax.fori_loop(0, blocks, place, 0)


def call(kernel, operands, specs, outs, out_specs, flops, scratch=(), limit=None, **kw):
    space = 0
    for x in (*operands, *outs, *scratch):
        space += x.size * x.dtype.itemsize if hasattr(x, "size") else 0
    moved = sum(x.size * x.dtype.itemsize for x in (*operands, *outs))
    semantics = {"dimension_semantics": ("arbitrary",)} if "grid" in kw else {}
    return pl.pallas_call(
        kernel,
        out_shape=tuple(outs),
        in_specs=specs,
        out_specs=tuple(out_specs),
        scratch_shapes=[pltpu.VMEM(x.shape, x.dtype) if isinstance(x, jax.ShapeDtypeStruct) else x for x in scratch],
        compiler_params=pltpu.CompilerParams(vmem_limit_bytes=int(limit or space + 3 * MIB), **semantics),
        cost_estimate=pl.CostEstimate(flops=int(flops), bytes_accessed=int(moved), transcendentals=0),
        **kw,
    )(*operands)


def in_hbm(x):
    return pltpu.with_memory_space_constraint(x, pltpu.HBM)


def shape(rows, columns, dtype):
    return jax.ShapeDtypeStruct((rows, columns), dtype)


def program(bounds, block_map, pivot_inverse, upper_block, lower_block, trailing_block, sketch, basis):
    fronts, row_count = lax.axis_size("front"), lax.axis_size("row")
    assert fronts % 4 == 0 and fronts & (fronts - 1) == 0
    blocks = block_map.shape[1]
    per_device = basis.shape[1] // BLOCK
    cap = -(-blocks // fronts)
    depth, width = sketch.shape
    half = width // 2
    ids = jnp.stack([lax.axis_index("front"), lax.axis_index("row"), lax.axis_index("col")]).astype(jnp.int32)
    inverse, upper, lower, trailing, basis = pivot_inverse[0], upper_block[0], lower_block[0], trailing_block[0], basis[0]
    height, _ = lower.shape
    tall = upper.shape[0]
    groups, cuts = groups_of(fronts, cap)

    steps = 5 if depth % (5 * BLOCK) == 0 else 1
    tile = 4 * BLOCK if height % (4 * BLOCK) == 0 else BLOCK
    head = max(height // tile * 2 // 5, 1) * tile
    send_own, send_other, kept_own, kept_other, masked, top, order, offset, tags = call(
        functools.partial(pivot_kernel, (row_count, per_device, cap, fronts)),
        (ids, bounds, in_hbm(block_map.reshape(-1)), in_hbm(upper), in_hbm(sketch), in_hbm(trailing)),
        [SMEM, SMEM, ANY, ANY, ANY, ANY],
        (shape(tall, half, BF16),) * 2
        + (shape(tall, half, F32),) * 2
        + (shape(depth, width, BF16), shape(head, depth, BF16))
        + tuple(jax.ShapeDtypeStruct((n,), jnp.int32) for n in (blocks, fronts + 1, fronts * cap + blocks)),
        [VMEM] * 6 + [SMEM] * 3,
        2 * upper.size * width,
        scratch=(
            shape(tall, depth, BF16),
            shape(depth, width, BF16),
            shape(tall, width, F32),
            pltpu.SemaphoreType.DMA((steps,)),
            pltpu.SemaphoreType.DMA((steps,)),
            pltpu.SemaphoreType.DMA,
            pltpu.SemaphoreType.DMA,
            pltpu.SMEM((blocks,), jnp.int32),
            pltpu.SMEM((fronts + 1,), jnp.int32),
            pltpu.SMEM((blocks,), jnp.int32),
            pltpu.SMEM((blocks,), jnp.int32),
        ),
    )
    got_other = swap(send_own, "col")
    got_own = swap(send_other, "col")

    trail_own, trail_other = call(
        functools.partial(trailing_kernel, tile),
        (in_hbm(trailing), top, masked),
        [ANY, VMEM, VMEM],
        (shape(height, half, F32),) * 2,
        [VMEM] * 2,
        2 * trailing.size * width,
        scratch=(shape(height - head, depth, BF16), pltpu.SemaphoreType.DMA(((height - head) // tile,))),
    )

    def solve(kept, got):
        return call(solve_kernel, (inverse, kept, got), [VMEM] * 3, (shape(inverse.shape[0], half, F32),), [VMEM], 2 * inverse.size * half)[0]

    part_other = solve(kept_other, got_other)
    row_other = swap(part_other, "row")
    cuts = [min(c, blocks) for c in cuts]
    counts = [b - a for a, b in zip(cuts, cuts[1:])]
    sums = call(
        first_schur_kernel,
        (order, part_other, row_other, lower, trail_other),
        [SMEM] + [VMEM] * 4,
        (shape(counts[0] * BLOCK, half, BF16),),
        [VMEM],
        2 * lower.size * half,
    )
    sums += call(
        functools.partial(packed_schur_kernel, [a for a, n in zip(cuts[1:], counts[1:]) if n]),
        (order, part_other, row_other, lower, trail_other),
        [SMEM] + [VMEM] * 4,
        tuple(shape(n * BLOCK, half, BF16) for n in counts[1:] if n),
        [VMEM] * sum(n > 0 for n in counts[1:]),
        2 * lower.size * half,
        scratch=(shape(height, half, BF16),),
    )
    arrived = [swap(x, "col") for x in sums]
    part_own = solve(kept_own, got_own)
    row_own = swap(part_own, "row")

    pieces = []
    total = None
    for g, parts in enumerate(groups):
        if not parts:
            continue
        operands = [order, offset, tags, part_own, row_own, lower, trail_own]
        if counts[g]:
            operands.append(arrived[g])
        if g:
            operands.append(total)
        total, *made = call(
            functools.partial(add_kernel, parts, cap, cuts[g], counts[g], g == 0),
            operands,
            [SMEM] * 3 + [VMEM] * (len(operands) - 3),
            (shape(blocks * BLOCK, half, BF16),)
            + tuple(shape((high - low) * BLOCK + TAG_ROWS, half, BF16) for _, low, high in parts),
            [VMEM] * (1 + len(parts)),
            1e9,
            **({"input_output_aliases": {len(operands) - 1: 0}} if g else {}),
        )
        for (key, _, _), piece in zip(parts, made):
            pieces.append(away(piece, key, fronts) if key < fronts - 1 else piece)

    rank = basis.shape[1]
    rows = per_device * BLOCK
    flipped = call(flip_kernel, (basis,), [VMEM], (shape(rank, rows, BF16),), [VMEM], 1e9)[0]
    inner, extra = fronts // 4, int(cap > 1)
    far = inner + extra
    late, middle = 2 * inner - 1 + extra, [len(pieces) - 2, 3 * inner - 1 + extra]
    waves = [[len(pieces) - 1] + list(range(far))]
    waves += [[i for i in range(far, len(pieces) - 2) if i not in (late, *middle)], middle, [late]]
    parent = None
    for w, keys in enumerate(waves[:-1]):
        parent = call(
            functools.partial(early_kernel, per_device, w == 0),
            [pieces[k] for k in keys] + ([parent] if w else []),
            [VMEM] * (len(keys) + (w > 0)),
            (shape(rows, half, F32),),
            [VMEM],
            1e9,
            **({"input_output_aliases": {len(keys): 0}} if w else {}),
        )[0]
    parent, coeff = call(
        functools.partial(late_kernel, per_device),
        [flipped, parent] + [pieces[k] for k in waves[-1]],
        [VMEM] * (2 + len(waves[-1])),
        (shape(rows, half, F32), shape(rank, half, F32)),
        [VMEM] * 2,
        2 * basis.size * half,
        input_output_aliases={1: 0},
    )
    got = swap(coeff, "row")
    steps = 6 if per_device % 6 == 0 else 1
    coefficients, residual = call(
        residual_kernel,
        (basis, parent, coeff, got),
        [VMEM] * 4,
        (shape(rank, half, F32), shape(rows, half, F32)),
        [ANY] * 2,
        2 * basis.size * half,
        scratch=(
            shape(rank, half, F32),
            shape(rows, half, F32),
            pltpu.SemaphoreType.DMA,
            pltpu.SemaphoreType.DMA((steps,)),
        ),
    )
    return coefficients[None], residual[None]


def solution(mesh):
    placed = (
        P("front"),
        P("front", "row"),
        P("front", "col", "row"),
        P("front", "row", "col"),
        P("front", "row", "col"),
        P("front", "row", "col"),
        P("col", None),
        P("front", "row", None),
    )

    def step(*args):
        sharded = jax.shard_map(
            program,
            mesh=mesh,
            in_specs=placed,
            out_specs=(P("front", None, "col"), P("front", "row", "col")),
            check_vma=False,
        )
        return sharded(*args)

    return step
```

```python
import functools

import jax
import jax.numpy as jnp
from jax import lax
from jax.experimental import pallas as pl
from jax.experimental.pallas import tpu as pltpu
from jax.sharding import PartitionSpec as P


BLOCK = 128
TAG_ROWS = 8
F32 = jnp.float32
BF16 = jnp.bfloat16
VMEM = pl.BlockSpec(memory_space=pltpu.VMEM)
SMEM = pl.BlockSpec(memory_space=pltpu.SMEM)
MIB = 1024 * 1024
ANY = pl.BlockSpec(memory_space=pl.ANY)


def dot(a, b):
    return jnp.dot(a, b, preferred_element_type=F32)


def pivot_kernel(
    sizes, ids_ref, bound_ref, map_hbm, upper_hbm, sketch_hbm, trailing_hbm,
    own_ref, other_ref, kept_own_ref, kept_other_ref, masked_ref, head_ref, order_ref, offset_ref, tag_ref,
    upper_ref, sketch_ref, sum_ref, upper_sem, sketch_sem, head_sem, map_sem, map_ref, count_ref, rank_ref, key_ref,
):
    map_copy = pltpu.make_async_copy(map_hbm, map_ref, map_sem)
    map_copy.start()
    depth, width = sketch_ref.shape
    half = width // 2
    parts = upper_sem.shape[0]
    part = depth // parts
    copies = []
    for k in range(parts):
        at = pl.ds(k * part, part)
        copies.append(
            (
                pltpu.make_async_copy(upper_hbm.at[:, at], upper_ref.at[:, at], upper_sem.at[k]),
                pltpu.make_async_copy(sketch_hbm.at[at, :], sketch_ref.at[at, :], sketch_sem.at[k]),
            )
        )
        for copy in copies[-1]:
            copy.start()
    head_copy = pltpu.make_async_copy(trailing_hbm.at[pl.ds(0, head_ref.shape[0]), :], head_ref, head_sem)
    head_copy.start()
    map_copy.wait()
    plan(*sizes, ids_ref, bound_ref, map_ref, order_ref, offset_ref, tag_ref, count_ref, rank_ref, key_ref)
    col = ids_ref[2]
    for k in range(parts):
        for copy in copies[k]:
            copy.wait()
        for start in range(k * part, (k + 1) * part, BLOCK):
            rows = slice(start, start + BLOCK)
            keep = jnp.where(col * depth + start < bound_ref[0], 1.0, 0.0).astype(F32)
            keep = jnp.full((BLOCK, half), keep, F32).astype(BF16)
            for side in range(2):
                pick = col if side == 0 else 1 - col
                value = sketch_ref[rows, pl.ds(pl.multiple_of(pick * half, half), half)]
                masked_ref[rows, side * half : (side + 1) * half] = value * keep
        first = (parts + 1) // 2
        if k == first - 1:
            at = slice(0, first * part)
            sum_ref[...] = dot(upper_ref[:, at], masked_ref[at, :])
        if k == parts - 1 and parts > 1:
            at = slice(first * part, depth)
            sum_ref[...] += dot(upper_ref[:, at], masked_ref[at, :])
    kept_own_ref[...] = sum_ref[:, :half]
    own_ref[...] = sum_ref[:, :half].astype(BF16)
    kept_other_ref[...] = sum_ref[:, half:]
    other_ref[...] = sum_ref[:, half:].astype(BF16)
    head_copy.wait()


def trailing_kernel(tile, trailing_hbm, head_ref, masked_ref, own_ref, other_ref, rest_ref, rest_sem):
    height, half = own_ref.shape
    head = head_ref.shape[0]
    copies = []
    for i, start in enumerate(range(head, height, tile)):
        copies.append(
            pltpu.make_async_copy(
                trailing_hbm.at[pl.ds(start, tile), :], rest_ref.at[pl.ds(start - head, tile), :], rest_sem.at[i]
            )
        )
        copies[-1].start()
    for start in range(0, height, tile):
        rows = slice(start, start + tile)
        if start < head:
            value = dot(head_ref[rows, :], masked_ref[...])
        else:
            copies[(start - head) // tile].wait()
            value = dot(rest_ref[start - head : start - head + tile, :], masked_ref[...])
        own_ref[rows, :] = value[:, :half]
        other_ref[rows, :] = value[:, half:]


def solve_kernel(inverse_ref, kept_ref, got_ref, out_ref):
    rows = (kept_ref[...] + got_ref[...].astype(F32)).astype(BF16)
    out_ref[...] = dot(inverse_ref[...], rows)


def schur_kernel(part_ref, got_ref, lower_ref, trailing_ref, out_ref):
    solved = (part_ref[...] + got_ref[...]).astype(BF16)
    height = lower_ref.shape[0]
    step = 4 * BLOCK if height % (4 * BLOCK) == 0 else BLOCK
    for start in range(0, height, step):
        rows = slice(start, start + step)
        out_ref[rows, :] = (trailing_ref[rows, :] - dot(lower_ref[rows, :], solved)).astype(out_ref.dtype)


def first_schur_kernel(order_ref, part_ref, got_ref, lower_ref, trailing_ref, out_ref):
    solved = (part_ref[...] + got_ref[...]).astype(BF16)
    for p in range(out_ref.shape[0] // BLOCK):
        at = pl.ds(pl.multiple_of(order_ref[p] * BLOCK, BLOCK), BLOCK)
        value = trailing_ref[at, :] - dot(lower_ref[at, :], solved)
        out_ref[p * BLOCK : (p + 1) * BLOCK, :] = value.astype(BF16)


def packed_schur_kernel(cuts, order_ref, part_ref, got_ref, lower_ref, trailing_ref, *rest):
    outs, sum_ref = rest[:-1], rest[-1]
    schur_kernel(part_ref, got_ref, lower_ref, trailing_ref, sum_ref)
    for out, first in zip(outs, cuts):
        for p in range(out.shape[0] // BLOCK):
            at = pl.multiple_of(order_ref[first + p] * BLOCK, BLOCK)
            out[p * BLOCK : (p + 1) * BLOCK, :] = sum_ref[pl.ds(at, BLOCK), :]


def add_kernel(
    parts, cap, first, count, fresh, order_ref, offset_ref, tag_ref, part_ref, row_ref, lower_ref, trailing_ref, *refs
):
    refs = list(refs)
    got_ref = refs.pop(0) if count else None
    if not fresh:
        refs.pop(0)
    sum_ref, outs = refs[0], refs[1:]
    solved = (part_ref[...] + row_ref[...]).astype(BF16)
    for p in range(count):
        at = pl.ds(pl.multiple_of(order_ref[first + p] * BLOCK, BLOCK), BLOCK)
        value = trailing_ref[at, :] - dot(lower_ref[at, :], solved) + got_ref[p * BLOCK : (p + 1) * BLOCK, :].astype(F32)
        sum_ref[(first + p) * BLOCK : (first + p + 1) * BLOCK, :] = value.astype(BF16)
    last = sum_ref.shape[0] // BLOCK - 1
    index = lax.broadcasted_iota(jnp.int32, (TAG_ROWS, sum_ref.shape[1]), 0)
    for (key, low, high), out in zip(parts, outs):
        tags = jnp.zeros(index.shape, F32)
        for s in range(low, high):
            at = pl.multiple_of(jnp.minimum(offset_ref[key] + s, last) * BLOCK, BLOCK)
            out[(s - low) * BLOCK : (s - low + 1) * BLOCK, :] = sum_ref[pl.ds(at, BLOCK), :]
            tags = jnp.where(index == s - low, tag_ref[key * cap + s].astype(F32), tags)
        out[(high - low) * BLOCK :, :] = tags.astype(BF16)


def add_pieces(per_device, pieces, parent_ref, rounded_ref=None):
    for piece in pieces:
        count = piece.shape[0] // BLOCK
        tile = piece[count * BLOCK : count * BLOCK + TAG_ROWS, :BLOCK].astype(F32)
        index = lax.broadcasted_iota(jnp.int32, tile.shape, 0)
        for s in range(count):
            tag = jnp.max(jnp.where(index == s, tile, 0.0)).astype(jnp.int32)

            @pl.when(tag < per_device)
            def _():
                at = pl.ds(pl.multiple_of(tag * BLOCK, BLOCK), BLOCK)
                parent_ref[at, :] += piece[s * BLOCK : (s + 1) * BLOCK, :].astype(F32)
                if rounded_ref is not None:
                    rounded_ref[at, :] = parent_ref[at, :].astype(BF16)


def early_kernel(per_device, fresh, *refs):
    pieces, parent_ref = refs[: -1 if fresh else -2], refs[-1]
    if fresh:
        parent_ref[...] = jnp.zeros_like(parent_ref)
    add_pieces(per_device, pieces, parent_ref)


def middle_kernel(per_device, *refs):
    pieces, (parent_ref, rounded_ref) = refs[:-3], refs[-2:]
    add_pieces(per_device, pieces, parent_ref)
    rounded_ref[...] = parent_ref[...].astype(BF16)


def late_kernel(per_device, *refs):
    flipped_ref, pieces, (parent_ref, rounded_ref, coeff_ref) = refs[0], refs[3:-3], refs[-3:]
    add_pieces(per_device, pieces, parent_ref, rounded_ref)
    coeff_ref[...] = dot(flipped_ref[...], rounded_ref[...])


def flip_kernel(basis_ref, out_ref):
    out_ref[...] = basis_ref[...].T


def residual_kernel(basis_ref, parent_ref, part_ref, got_ref, coeff_hbm, out_hbm, coeff_ref, out_ref, coeff_sem, out_sem):
    total = part_ref[...] + got_ref[...]
    coeff_ref[...] = total
    copies = [pltpu.make_async_copy(coeff_ref, coeff_hbm, coeff_sem)]
    total = total.astype(BF16)
    parts = out_sem.shape[0]
    part = out_ref.shape[0] // parts
    for k in range(parts):
        rows = slice(k * part, (k + 1) * part)
        out_ref[rows, :] = parent_ref[rows, :] - dot(basis_ref[rows, :], total)
        at = pl.ds(k * part, part)
        copies.append(pltpu.make_async_copy(out_ref.at[at, :], out_hbm.at[at, :], out_sem.at[k]))
        copies[-1].start()
        if k == 0:
            copies[0].start()
    for copy in copies:
        copy.wait()


def swap(x, axis):
    return lax.ppermute(x, axis, [(i, i ^ 1) for i in range(lax.axis_size(axis))])


def away(x, key, fronts):
    return lax.ppermute(
        x, "front", [(i, j) for i in range(fronts) for j in range(fronts) if key_of(j, i, fronts) == key]
    )


def groups_of(fronts, cap):
    total = fronts * cap
    cuts = [0, 2, total // 8, total // 4, 3 * total // 8, total // 2, 3 * total // 4, total]
    groups = []
    for a, b in zip(cuts, cuts[1:]):
        keys = range(a // cap, -(-b // cap))
        groups.append([(k, max(a - k * cap, 0), min(b - k * cap, cap)) for k in keys if b > a])
    return groups, cuts


LEGS = (2, 1, 3, 0)


def gray(x):
    return x ^ (x >> 1)


def key_of(owner, me, fronts):
    inner = fronts // 4
    leg = (gray(owner // inner) - gray(me // inner)) & 3 if isinstance(owner, int) else lax.bitwise_and(
        gray_of(lax.div(owner, inner)) - gray_of(lax.div(me, inner)) + 4, 3
    )
    rest = inner - 1 - ((owner ^ me) & (inner - 1))
    if isinstance(owner, int):
        return LEGS.index(leg) * inner + rest
    turn = jnp.where(leg == LEGS[0], 0, jnp.where(leg == LEGS[1], 1, jnp.where(leg == LEGS[2], 2, 3)))
    return turn * inner + rest


def gray_of(x):
    return lax.bitwise_xor(x, lax.shift_right_logical(x, jnp.int32(1)))


def divider(by, top):
    for shift in range(8, 31):
        factor = -(-(1 << shift) // by)
        if all(n * factor >> shift == n // by for n in range(top + 1)):
            assert top * factor < 1 << 31
            return factor, shift
    raise ValueError(by)


def plan(row_count, per_device, cap, fronts, ids_ref, bound_ref, map_ref, order_ref, offset_ref, tag_ref, count_ref, rank_ref, key_ref):
    me, row = ids_ref[0], ids_ref[1]
    blocks = map_ref.shape[0]
    factor, shift = divider(per_device, fronts * row_count * per_device)
    assert row_count & (row_count - 1) == 0
    inner = fronts // 4

    def zero(i, carry):
        count_ref[i] = 0
        return carry

    def no_tag(i, carry):
        tag_ref[i] = per_device
        return carry

    def rank_one(j, carry):
        value = map_ref[j]
        holder = lax.shift_right_logical(value * factor, jnp.int32(shift))
        owner = lax.shift_right_logical(holder, jnp.int32(row_count.bit_length() - 1))
        there, here = (lax.shift_right_logical(x, jnp.int32(inner.bit_length() - 1)) for x in (owner, me))
        there, here = (lax.bitwise_xor(x, lax.shift_right_logical(x, jnp.int32(1))) for x in (there, here))
        leg = lax.bitwise_and(there - here, jnp.int32(3))
        turn = jnp.where(leg == LEGS[0], 0, jnp.where(leg == LEGS[1], 1, jnp.where(leg == LEGS[2], 2, 3)))
        key = turn * inner + (inner - 1) - lax.bitwise_and(lax.bitwise_xor(owner, me), jnp.int32(inner - 1))
        key = jnp.where((row * blocks + j) * BLOCK < bound_ref[0], key, fronts)
        rank = count_ref[key]
        count_ref[key] = rank + 1
        rank_ref[j] = rank
        key_ref[j] = key
        tag_ref[key * cap + rank] = value - holder * per_device
        return carry

    def start(i, total):
        offset_ref[i] = total
        return total + count_ref[i]

    def place(j, carry):
        order_ref[offset_ref[key_ref[j]] + rank_ref[j]] = j
        return carry

    lax.fori_loop(0, fronts + 1, zero, 0)
    lax.fori_loop(0, fronts * cap, no_tag, 0)
    lax.fori_loop(0, blocks, rank_one, 0)
    lax.fori_loop(0, fronts + 1, start, jnp.int32(0))
    lax.fori_loop(0, blocks, place, 0)


def call(kernel, operands, specs, outs, out_specs, flops, scratch=(), limit=None, **kw):
    space = 0
    for x in (*operands, *outs, *scratch):
        space += x.size * x.dtype.itemsize if hasattr(x, "size") else 0
    moved = sum(x.size * x.dtype.itemsize for x in (*operands, *outs))
    semantics = {"dimension_semantics": ("arbitrary",)} if "grid" in kw else {}
    return pl.pallas_call(
        kernel,
        out_shape=tuple(outs),
        in_specs=specs,
        out_specs=tuple(out_specs),
        scratch_shapes=[pltpu.VMEM(x.shape, x.dtype) if isinstance(x, jax.ShapeDtypeStruct) else x for x in scratch],
        compiler_params=pltpu.CompilerParams(vmem_limit_bytes=int(limit or space + 3 * MIB), **semantics),
        cost_estimate=pl.CostEstimate(flops=int(flops), bytes_accessed=int(moved), transcendentals=0),
        **kw,
    )(*operands)


def in_hbm(x):
    return pltpu.with_memory_space_constraint(x, pltpu.HBM)


def shape(rows, columns, dtype):
    return jax.ShapeDtypeStruct((rows, columns), dtype)


def program(bounds, block_map, pivot_inverse, upper_block, lower_block, trailing_block, sketch, basis):
    fronts, row_count = lax.axis_size("front"), lax.axis_size("row")
    assert fronts % 4 == 0 and fronts & (fronts - 1) == 0
    blocks = block_map.shape[1]
    per_device = basis.shape[1] // BLOCK
    cap = -(-blocks // fronts)
    depth, width = sketch.shape
    half = width // 2
    ids = jnp.stack([lax.axis_index("front"), lax.axis_index("row"), lax.axis_index("col")]).astype(jnp.int32)
    inverse, upper, lower, trailing, basis = pivot_inverse[0], upper_block[0], lower_block[0], trailing_block[0], basis[0]
    height, _ = lower.shape
    tall = upper.shape[0]
    groups, cuts = groups_of(fronts, cap)

    steps = 5 if depth % (5 * BLOCK) == 0 else 1
    tile = 4 * BLOCK if height % (4 * BLOCK) == 0 else BLOCK
    head = max(height // tile * 2 // 5, 1) * tile
    send_own, send_other, kept_own, kept_other, masked, top, order, offset, tags = call(
        functools.partial(pivot_kernel, (row_count, per_device, cap, fronts)),
        (ids, bounds, in_hbm(block_map.reshape(-1)), in_hbm(upper), in_hbm(sketch), in_hbm(trailing)),
        [SMEM, SMEM, ANY, ANY, ANY, ANY],
        (shape(tall, half, BF16),) * 2
        + (shape(tall, half, F32),) * 2
        + (shape(depth, width, BF16), shape(head, depth, BF16))
        + tuple(jax.ShapeDtypeStruct((n,), jnp.int32) for n in (blocks, fronts + 1, fronts * cap + blocks)),
        [VMEM] * 6 + [SMEM] * 3,
        2 * upper.size * width,
        scratch=(
            shape(tall, depth, BF16),
            shape(depth, width, BF16),
            shape(tall, width, F32),
            pltpu.SemaphoreType.DMA((steps,)),
            pltpu.SemaphoreType.DMA((steps,)),
            pltpu.SemaphoreType.DMA,
            pltpu.SemaphoreType.DMA,
            pltpu.SMEM((blocks,), jnp.int32),
            pltpu.SMEM((fronts + 1,), jnp.int32),
            pltpu.SMEM((blocks,), jnp.int32),
            pltpu.SMEM((blocks,), jnp.int32),
        ),
    )
    got_other = swap(send_own, "col")
    got_own = swap(send_other, "col")

    trail_own, trail_other = call(
        functools.partial(trailing_kernel, tile),
        (in_hbm(trailing), top, masked),
        [ANY, VMEM, VMEM],
        (shape(height, half, F32),) * 2,
        [VMEM] * 2,
        2 * trailing.size * width,
        scratch=(shape(height - head, depth, BF16), pltpu.SemaphoreType.DMA(((height - head) // tile,))),
    )

    def solve(kept, got):
        return call(solve_kernel, (inverse, kept, got), [VMEM] * 3, (shape(inverse.shape[0], half, F32),), [VMEM], 2 * inverse.size * half)[0]

    part_other = solve(kept_other, got_other)
    row_other = swap(part_other, "row")
    cuts = [min(c, blocks) for c in cuts]
    counts = [b - a for a, b in zip(cuts, cuts[1:])]
    sums = call(
        first_schur_kernel,
        (order, part_other, row_other, lower, trail_other),
        [SMEM] + [VMEM] * 4,
        (shape(counts[0] * BLOCK, half, BF16),),
        [VMEM],
        2 * lower.size * half,
    )
    sums += call(
        functools.partial(packed_schur_kernel, [a for a, n in zip(cuts[1:], counts[1:]) if n]),
        (order, part_other, row_other, lower, trail_other),
        [SMEM] + [VMEM] * 4,
        tuple(shape(n * BLOCK, half, BF16) for n in counts[1:] if n),
        [VMEM] * sum(n > 0 for n in counts[1:]),
        2 * lower.size * half,
        scratch=(shape(height, half, BF16),),
    )
    arrived = [swap(x, "col") for x in sums]
    part_own = solve(kept_own, got_own)
    row_own = swap(part_own, "row")

    pieces = []
    total = None
    for g, parts in enumerate(groups):
        if not parts:
            continue
        operands = [order, offset, tags, part_own, row_own, lower, trail_own]
        if counts[g]:
            operands.append(arrived[g])
        if g:
            operands.append(total)
        total, *made = call(
            functools.partial(add_kernel, parts, cap, cuts[g], counts[g], g == 0),
            operands,
            [SMEM] * 3 + [VMEM] * (len(operands) - 3),
            (shape(blocks * BLOCK, half, BF16),)
            + tuple(shape((high - low) * BLOCK + TAG_ROWS, half, BF16) for _, low, high in parts),
            [VMEM] * (1 + len(parts)),
            1e9,
            **({"input_output_aliases": {len(operands) - 1: 0}} if g else {}),
        )
        for (key, _, _), piece in zip(parts, made):
            pieces.append(away(piece, key, fronts) if key < fronts - 1 else piece)

    rank = basis.shape[1]
    rows = per_device * BLOCK
    flipped = call(flip_kernel, (basis,), [VMEM], (shape(rank, rows, BF16),), [VMEM], 1e9)[0]
    inner, extra = fronts // 4, int(cap > 1)
    far = inner + extra
    late, middle = 2 * inner - 1 + extra, [len(pieces) - 2, 3 * inner - 1 + extra]
    waves = [[len(pieces) - 1] + list(range(far))]
    waves += [[i for i in range(far, len(pieces) - 2) if i not in (late, *middle)], middle, [late]]
    parent = None
    for w, keys in enumerate(waves[:-2]):
        parent = call(
            functools.partial(early_kernel, per_device, w == 0),
            [pieces[k] for k in keys] + ([parent] if w else []),
            [VMEM] * (len(keys) + (w > 0)),
            (shape(rows, half, F32),),
            [VMEM],
            1e9,
            **({"input_output_aliases": {len(keys): 0}} if w else {}),
        )[0]
    parent, rounded = call(
        functools.partial(middle_kernel, per_device),
        [pieces[k] for k in waves[-2]] + [parent],
        [VMEM] * (1 + len(waves[-2])),
        (shape(rows, half, F32), shape(rows, half, BF16)),
        [VMEM] * 2,
        1e9,
        input_output_aliases={len(waves[-2]): 0},
    )
    parent, _, coeff = call(
        functools.partial(late_kernel, per_device),
        [flipped, parent, rounded] + [pieces[k] for k in waves[-1]],
        [VMEM] * (3 + len(waves[-1])),
        (shape(rows, half, F32), shape(rows, half, BF16), shape(rank, half, F32)),
        [VMEM] * 3,
        2 * basis.size * half,
        input_output_aliases={1: 0, 2: 1},
    )
    got = swap(coeff, "row")
    steps = 8 if per_device % 8 == 0 else 1
    coefficients, residual = call(
        residual_kernel,
        (basis, parent, coeff, got),
        [VMEM] * 4,
        (shape(rank, half, F32), shape(rows, half, F32)),
        [ANY] * 2,
        2 * basis.size * half,
        scratch=(
            shape(rank, half, F32),
            shape(rows, half, F32),
            pltpu.SemaphoreType.DMA,
            pltpu.SemaphoreType.DMA((steps,)),
        ),
    )
    return coefficients[None], residual[None]


def solution(mesh):
    placed = (
        P("front"),
        P("front", "row"),
        P("front", "col", "row"),
        P("front", "row", "col"),
        P("front", "row", "col"),
        P("front", "row", "col"),
        P("col", None),
        P("front", "row", None),
    )

    def step(*args):
        sharded = jax.shard_map(
            program,
            mesh=mesh,
            in_specs=placed,
            out_specs=(P("front", None, "col"), P("front", "row", "col")),
            check_vma=False,
        )
        return sharded(*args)

    return step
```
